256 devices in a mesh: section: 16 (over y, x_hi, core), ctx: 16 (over z, x_lo).
Axes of the slice: x: 4 (x_hi: 2, x_lo: 2; x = x_hi * 2 + x_lo), y: 4, z: 8, core: 2. Of those that a mesh axis runs over, the one named last changes fastest.
Arguments:
- section_inputs: bfloat16 [16, 1792, 2048], P('section', 'ctx'), may hold values from -3 to 3
- saved_inputs: bfloat16 [16, 1792, 2048], P('section', 'ctx'), may hold values from -3 to 3
- output_grads: bfloat16 [16, 1792, 2048], P('section', 'ctx'), may hold values from -6 to 6
- token_positions: int32 [1792], P('ctx'), may hold values from 0 to 1791, each once
- norm_gain: float32 [16, 2048], P('section'), may hold values from 0.7 to 6
- query_weight: bfloat16 [16, 2048, 2048], P('section', 'ctx'), may hold values from -0.13258252 to 0.13258252
- keyval_weight: bfloat16 [16, 2048, 1024], P('section', 'ctx'), may hold values from -0.13258252 to 0.13258252
- output_weight: bfloat16 [16, 2048, 2048], P('section'), may hold values from -0.125 to 0.125
Outputs:
- next_inputs: bfloat16 [16, 1792, 2048], P('section', 'ctx')
- input_grads: bfloat16 [16, 1792, 2048], P('section', 'ctx')
The draws below stay inside these ranges and needn't reach their ends.
Inputs may be any that keep to these rules, and one draw needn't show every extreme that they name: `token_positions`: each position of the sequence once.
All inputs are finite; a program needn't handle non-finite values.
Results may differ from the reference program's by a relative error of at most 0.04.
The reference program's roundings to bfloat16 on the way (of `normed`, `rounded` and `mixed`) count: a program that leaves them out, or rounds other values in their place, can miss the bound.
Values may be sent and summed in bfloat16 or wider, within the bound.
A program may use at most 192 MiB of HBM per device.

```python
import jax
import jax.numpy as jnp
from jax import lax

D = 2048
HEADS = 16
KV_HEADS = 4
HEAD_DIM = 128
SECTIONS = 16
SEQ = 1792


def paired_weights(key):
    query_key = jax.random.fold_in(key, 11)
    keyval_key = jax.random.fold_in(key, 12)
    query_matrix = jax.random.truncated_normal(query_key, -4.0, 4.0, (SECTIONS, D, HEADS * HEAD_DIM), jnp.float32) * D ** (-0.5)
    keyval_matrix = jax.random.truncated_normal(keyval_key, -4.0, 4.0, (SECTIONS, D, 2 * KV_HEADS * HEAD_DIM), jnp.float32) * D ** (-0.5)
    return (query_matrix, keyval_matrix)


def draw_query_weight(key, part):
    return paired_weights(key)[0].astype(jnp.bfloat16)


def draw_keyval_weight(key, part):
    return paired_weights(key)[1].astype(jnp.bfloat16)


def draw_norm_gain(key, part):
    gain_key = jax.random.fold_in(key, 21)
    return 1.0 + 0.1 * jax.random.truncated_normal(gain_key, -3.0, 3.0, (SECTIONS, D), jnp.float32)


def block_levels(key, dims, shards, low, top_value):
    level, own = 1.0, jax.random.fold_in(key, 6)
    for axis_at, shards_of in shards:
        steps = jnp.exp(jax.random.uniform(jax.random.fold_in(own, axis_at), (shards_of,), jnp.float32, low / len(shards), top_value / len(shards)))
        level = level * jnp.repeat(steps, dims[axis_at] // shards_of).reshape([-1 if axis == axis_at else 1 for axis in range(len(dims))])
    return level


def normal_values(key, shape, spread, bound, cuts=(), kind=jnp.bfloat16):
    array = spread * jax.random.normal(key, shape, jnp.float32)
    if cuts:
        array = array * block_levels(key, shape, cuts, -0.22, 0.18)
    return jnp.clip(array, -bound, bound).astype(kind)


def setup_inputs(seed: int = 0) -> dict:
    keys = jax.random.split(jax.random.key(seed), 9)
    section_inputs = normal_values(keys[0], (SECTIONS, SEQ, D), 0.5, 3.0, ((0, 16), (1, 16)))
    saved_inputs = normal_values(keys[1], (SECTIONS, SEQ, D), 0.5, 3.0, ((0, 16), (1, 16)))
    output_grads = normal_values(keys[2], (SECTIONS, SEQ, D), 1.0, 6.0, ((0, 16), (1, 16)))
    token_positions = jax.random.permutation(keys[3], SEQ).astype(jnp.int32)
    norm_gain = draw_norm_gain(jax.random.fold_in(keys[8], 71), 0)
    query_weight = draw_query_weight(jax.random.fold_in(keys[8], 71), 0)
    keyval_weight = draw_keyval_weight(jax.random.fold_in(keys[8], 71), 0)
    output_weight = normal_values(keys[7], (SECTIONS, HEADS * HEAD_DIM, D), (HEADS * HEAD_DIM) ** -0.5, 0.125, ((0, 16),))
    return {"section_inputs": section_inputs, "saved_inputs": saved_inputs, "output_grads": output_grads, "token_positions": token_positions, "norm_gain": norm_gain, "query_weight": query_weight, "keyval_weight": keyval_weight, "output_weight": output_weight}


norm_eps = 1e-05
rope_base = 500000.0

def rotate(matrix, positions):
    half_dim = matrix.shape[-1] // 2
    frequency = rope_base ** (-2.0 * jnp.arange(half_dim, dtype=jnp.float32) / matrix.shape[-1])
    angles = positions.astype(jnp.float32)[:, None] * frequency[None, :]
    cos_table = jnp.cos(angles)[:, None, :]
    sin_table = jnp.sin(angles)[:, None, :]
    leading = matrix[..., :half_dim]
    trailing = matrix[..., half_dim:]
    return jnp.concatenate([leading * cos_table - trailing * sin_table, trailing * cos_table + leading * sin_table], axis=-1)

def project(tokens, gain, query_matrix, keyval_matrix, positions):
    widened = tokens.astype(jnp.float32)
    inverse = lax.rsqrt(lax.optimization_barrier(jnp.mean(widened * widened, axis=-1, keepdims=True)) + norm_eps)
    normed = (widened * inverse * gain[None, :]).astype(jnp.bfloat16)
    row_count = tokens.shape[0]
    query_full = jnp.dot(normed, query_matrix, preferred_element_type=jnp.float32)
    keyval_full = jnp.dot(normed, keyval_matrix, preferred_element_type=jnp.float32)
    queries = rotate(query_full.reshape(row_count, -1, HEAD_DIM), positions).astype(jnp.bfloat16)
    paired = keyval_full.reshape(row_count, 2, -1, HEAD_DIM)
    key_rows = rotate(paired[:, 0], positions).astype(jnp.bfloat16)
    value_rows = paired[:, 1].astype(jnp.bfloat16)
    return (queries, key_rows, value_rows)

def attend(queries, key_wide, value_wide, query_pos, key_pos):
    row_count = queries.shape[0]
    group_size = queries.shape[1] // key_wide.shape[1]
    grouped = queries.astype(jnp.float32).reshape(row_count, key_wide.shape[1], group_size, queries.shape[2])
    scores = jnp.einsum('rkgd,skd->kgrs', grouped, key_wide) * queries.shape[2] ** (-0.5)
    visible = (key_pos[None, :] <= query_pos[:, None])[None, None]
    masked = jnp.where(visible, scores, -1e+30)
    row_max = lax.stop_gradient(lax.optimization_barrier(jnp.max(masked, axis=-1, keepdims=True)))
    numerators = jnp.where(visible, jnp.exp(masked - row_max), 0.0)
    totals = lax.optimization_barrier(jnp.sum(numerators, axis=-1))
    rounded = lax.optimization_barrier(numerators.astype(jnp.bfloat16)).astype(jnp.float32)
    summed = jnp.einsum('kgrs,skd->rkgd', rounded, value_wide)
    averaged = summed / jnp.transpose(totals, (2, 0, 1))[..., None]
    return averaged.reshape(row_count, -1).astype(jnp.bfloat16)

def finish(tokens, mixed, output_matrix):
    return (tokens.astype(jnp.float32) + jnp.dot(mixed, output_matrix, preferred_element_type=jnp.float32)).astype(jnp.bfloat16)

def section_layer(tokens, gain, query_matrix, keyval_matrix, output_matrix, positions):
    queries, key_rows, value_rows = project(tokens, gain, query_matrix, keyval_matrix, positions)
    mixed = attend(queries, key_rows.astype(jnp.float32), value_rows.astype(jnp.float32), positions, positions)
    return finish(tokens, mixed, output_matrix)

def reference(section_inputs, saved_inputs, output_grads, token_positions, norm_gain, query_weight, keyval_weight, output_weight):

    def one_section(packed):
        forward_tokens, saved_tokens, upstream, gain, query_matrix, keyval_matrix, output_matrix = packed

        def layer(tokens):
            return section_layer(tokens, gain, query_matrix, keyval_matrix, output_matrix, token_positions)
        produced = layer(forward_tokens)
        unused, back_layer = jax.vjp(layer, saved_tokens)
        token_grads, = back_layer(upstream)
        return (produced, token_grads)
    results, gradients = lax.map(one_section, (section_inputs, saved_inputs, output_grads, norm_gain, query_weight, keyval_weight, output_weight))
    return (jnp.roll(results, 1, axis=0), jnp.roll(gradients, -1, axis=0))
```

```python
import functools

import jax
import jax.numpy as jnp
from jax import lax
from jax.experimental import pallas as pl
from jax.experimental.pallas import tpu as pltpu
from jax.sharding import PartitionSpec as P

MESH = pl.DeviceIdType.MESH
F32 = jnp.float32
BF16 = jnp.bfloat16
HEAD_DIM = 128
LANES = 256
norm_eps = 1e-05
rope_base = 500000.0
LOG2E = 1.4426950408889634
HIDDEN = -1e30


def dot(a, b):
    return jnp.dot(a, b, preferred_element_type=F32)


def dot_nt(a, b):
    return lax.dot_general(a, b, (((1,), (1,)), ((), ())), preferred_element_type=F32)


def fold_rows(a, op):
    return op(a.reshape(a.shape[0] // 8, 8, a.shape[1]), axis=0)


def tick(
    planes,
    rows,
    xs_in,
    xf_in,
    dy_in,
    pos_in,
    tab_in,
    gain_in,
    wq_hbm,
    wkv_hbm,
    wo_hbm,
    next_out,
    grad_out,
    wbuf,
    wo,
    xbuf,
    tabs,
    posb,
    normed,
    acc,
    qnat,
    qt,
    kv,
    kvt,
    dkv,
    bias,
    qpos,
    dmt,
    score,
    prob,
    dsc,
    stage,
    landed,
    mix,
    mixed,
    dqkv,
    dnsend,
    dnrecv,
    dnown,
    loc_sem,
    x_send,
    x_recv,
    w_send,
    w_recv,
    pos_send,
    pos_recv,
    kv_send,
    kv_recv,
    rs_send,
    rs_recv,
):
    me = lax.axis_index("ctx")
    z = me // 2
    h = me % 2
    partner = z * 2 + 1 - h
    up = ((z + 1) % planes) * 2 + h
    down = ((z + planes - 1) % planes) * 2 + h
    width = wbuf.shape[2]
    half = width // 2
    pair = 2 * rows
    keys = planes * pair
    chunk = 256
    chunks = keys // chunk
    mine = pl.ds(pl.multiple_of(h * rows, 16), rows)
    theirs = pl.ds(pl.multiple_of((1 - h) * rows, 16), rows)
    to_z = (up, down)
    scale = HEAD_DIM ** (-0.5)

    barrier = pltpu.get_barrier_semaphore()
    for other in (partner, up, down):
        pl.semaphore_signal(barrier, inc=1, device_id={"ctx": other}, device_id_type=MESH)

    def local(src, dst, n):
        return pltpu.make_async_copy(src, dst, loc_sem.at[n])

    def remote(src, dst, s, r, to):
        return pltpu.make_async_remote_copy(
            src_ref=src, dst_ref=dst, send_sem=s, recv_sem=r, device_id={"ctx": to}, device_id_type=MESH
        )

    def to_partner(src, dst, n):
        return remote(src, dst, x_send.at[n], x_recv.at[n], partner)

    def pieces(side):
        out = []
        for j in range(2):
            g = 2 * side + j
            wide = pl.ds(pl.multiple_of(g * 512, 512), 512)
            key = pl.ds(pl.multiple_of(g * 128, 128), 128)
            value = pl.ds(pl.multiple_of(512 + g * 128, 128), 128)
            out.append((wq_hbm.at[:, wide], j, pl.ds(0, 512)))
            out.append((wkv_hbm.at[:, key], j, pl.ds(512, 128)))
            out.append((wkv_hbm.at[:, value], j, pl.ds(640, 128)))
        return out

    my_rows = pl.ds(pl.multiple_of(h * half, 128), half)
    own = [local(src, wbuf.at[j, z, my_rows, cols], n) for n, (src, j, cols) in enumerate(pieces(h))]
    for c in own:
        c.start()
    load_wo = local(wo_hbm, wo, 6)
    load_wo.start()
    keep_pos = local(pos_in, posb.at[me], 7)
    keep_pos.start()

    for n in range(3):
        xbuf[n, pl.ds(pair, LANES - pair), :] = jnp.zeros((LANES - pair, xbuf.shape[2]), BF16)
    for n in range(2):
        tabs[n, pl.ds(pair, LANES - pair), :] = jnp.zeros((LANES - pair, HEAD_DIM), F32)

    pl.semaphore_wait(barrier, 3)

    swap = [
        to_partner(pos_in, posb.at[me], 0),
        to_partner(tab_in, tabs.at[:, mine, :], 1),
    ]
    for n, (src, j, cols) in enumerate(pieces(1 - h)):
        swap.append(to_partner(src, wbuf.at[j, z, my_rows, cols], 2 + n))
    for n, src in enumerate((xs_in, xf_in, dy_in)):
        swap.append(to_partner(src, xbuf.at[n, mine, :], 8 + n))
    for c in swap:
        c.start()

    def w_copy(j, t, c):
        p = (z + planes - t) % planes if j == 0 else (z + t) % planes
        who = h if c == 0 else 1 - h
        block = wbuf.at[j, p, pl.ds(pl.multiple_of(who * half, 128), half), :]
        return remote(block, block, w_send.at[j, t, c], w_recv.at[j, t, c], to_z[j])

    def pos_copy(t):
        p = (z + planes - t) % planes
        block = posb.at[pl.ds(2 * p, 2)]
        return remote(block, block, pos_send.at[t], pos_recv.at[t], up)

    def w_step(t):
        for c in range(2):
            for j in range(2):
                if t > 0:
                    w_copy(j, t - 1, c).wait_recv()
                elif c == 0:
                    for n in range(3 * j, 3 * j + 3):
                        own[n].wait()
                else:
                    for n in range(3 * j, 3 * j + 3):
                        swap[2 + n].wait_recv()
                w_copy(j, t, c).start()
            if c == 0 and t == 0:
                for n, src in enumerate((xs_in, xf_in, dy_in)):
                    xbuf[n, mine, :] = src[...]
                tabs[:, mine, :] = tab_in[...]
            if c == 1:
                if t > 0:
                    pos_copy(t - 1).wait_recv()
                else:
                    keep_pos.wait()
                    swap[0].wait_recv()
                pos_copy(t).start()

    def norms():
        for n in range(2):
            def body(i, _):
                at = pl.ds(pl.multiple_of(i * 32, 32), 32)
                x = xbuf[n, at, :].astype(F32)
                inverse = lax.rsqrt(jnp.mean(x * x, axis=-1, keepdims=True) + norm_eps)
                y = (x * inverse * gain_in[...]).astype(BF16)
                for p in range(planes):
                    normed[p, pl.ds(pl.multiple_of(n * LANES + i * 32, 32), 32), :] = y[:, p * width : (p + 1) * width]
                return 0

            lax.fori_loop(0, LANES // 32, body, 0)

    def project(j, p, first):
        a = normed[p]
        if first:
            acc[j] = dot(a, wbuf[j, p])
        else:
            acc[j] += dot(a, wbuf[j, p])

    def grads_in():
        def body(n, _):
            at = pl.ds(pl.multiple_of(h * 1024 + n * 128, 128), 128)
            dmt[n] = dot_nt(wo[at, :], xbuf[2]).astype(BF16)
            return 0

        lax.fori_loop(0, 8, body, 0)

    for t in range(planes - 1):
        w_step(t)
        if t == 2:
            swap[1].wait_recv()
            swap[8].wait_recv()
            swap[9].wait_recv()
            norms()
            for j in range(2):
                project(j, z, True)
        if t == 3:
            for j in range(2):
                for s in (1, 2, 3):
                    p = (z + planes - s) % planes if j == 0 else (z + s) % planes
                    project(j, p, False)
        if t > 3:
            for j in range(2):
                p = (z + planes - t) % planes if j == 0 else (z + t) % planes
                project(j, p, False)
        if t == 4:
            load_wo.wait()
            swap[10].wait_recv()
            grads_in()
    t = planes - 1
    for c in range(2):
        for j in range(2):
            w_copy(j, t - 1, c).wait_recv()
    pos_copy(t - 1).wait_recv()
    for j in range(2):
        p = (z + planes - t) % planes if j == 0 else (z + t) % planes
        project(j, p, False)

    def rotated(x, sign):
        return x * tabs[0] + sign * (pltpu.roll(x, HEAD_DIM // 2, 1) * tabs[1])

    at_z = pl.ds(pl.multiple_of(z * pair, 32), pair)

    def make_kv(m):
        for j in range(2):
            a = acc.at[j, pl.ds(m * LANES, LANES), :]
            kv[m, j, 0, at_z, :] = rotated(a[:, 512:640], 1.0).astype(BF16)[:pair]
            kv[m, j, 1, at_z, :] = a[:, 640:768].astype(BF16)[:pair]

    def make_q(m):
        for j in range(2):
            a = acc.at[j, pl.ds(m * LANES, LANES), :]
            for r in range(4):
                q = rotated(a[:, r * 128 : r * 128 + 128], 1.0)
                if m == 0:
                    qnat[4 * j + r] = q.astype(BF16)
                qt[m, 4 * j + r] = q.T.astype(BF16)

    def kv_copy(m, j, k, t):
        p = (z + planes - t) % planes if j == 0 else (z + t) % planes
        block = kv.at[m, j, k, pl.ds(pl.multiple_of(p * pair, 32), pair), :]
        return remote(block, block, kv_send.at[m, j, k, t], kv_recv.at[m, j, k, t], to_z[j])

    def kv_start(m, t):
        for k in range(2):
            for j in range(2):
                kv_copy(m, j, k, t).start()

    def kv_step(m, t):
        for k in range(2):
            for j in range(2):
                kv_copy(m, j, k, t - 1).wait_recv()
                kv_copy(m, j, k, t).start()

    def make_bias():
        row0 = posb[2 * z][0:1, :]
        row1 = posb[2 * z + 1][0:1, :]
        zero = jnp.zeros_like(row0)
        wide0 = jnp.concatenate([row0, zero], axis=1)
        wide1 = pltpu.roll(jnp.concatenate([row1, zero], axis=1), rows, 1)
        lane = lax.broadcasted_iota(jnp.int32, (1, LANES), 1)
        query = jnp.where(lane < rows, wide0, jnp.where(lane < pair, wide1, 1e9))

        def body(i, _):
            column = jnp.broadcast_to(posb[i][0:1, :], (128, 128)).T
            column = jnp.concatenate([column, column], axis=1)[:rows]
            at = pl.ds(pl.multiple_of(i * rows, 16), rows)
            bias[at, :] = jnp.where(column <= query, 0.0, HIDDEN)
            return 0

        lax.fori_loop(0, 2 * planes, body, 0)

    def transposed(m):
        for j in range(2):
            for k in range(2):
                def body(i, _):
                    at = pl.ds(pl.multiple_of(i * 128, 128), 128)
                    kvt[j, k, :, at] = kv[m, j, k, at, :].astype(F32).T.astype(BF16)
                    return 0

                lax.fori_loop(0, keys // 128, body, 0)

    def softmax(m, j, i):
        q = qt[m, i]
        top = jnp.full((8, LANES), HIDDEN, F32)
        for c in range(chunks):
            at = pl.ds(c * chunk, chunk)
            s = dot(kv[m, j, 0, at, :], q) + bias[at, :]
            score[at, :] = s
            top = jnp.maximum(top, fold_rows(s, jnp.max))
        top = jnp.max(top, axis=0, keepdims=True)
        total = jnp.zeros((8, LANES), F32)
        for c in range(chunks):
            at = pl.ds(c * chunk, chunk)
            e = jnp.exp2((score[at, :] - top) * (scale * LOG2E))
            total += fold_rows(e, jnp.sum)
            if m == 0:
                score[at, :] = e
            prob[at, :] = e.astype(BF16)
        return jnp.sum(total, axis=0, keepdims=True)

    def backward(i):
        j = i // 4
        inverse = 1.0 / softmax(0, j, i)
        summed = dot(kvt[j, 1], prob[...])
        dm = dmt[i].astype(F32)
        share = -jnp.sum(dm * summed, axis=0, keepdims=True) * (inverse * inverse)
        dsum = dm * inverse
        dsum_t = dsum.astype(BF16)
        dsum_n = dsum.T.astype(BF16)
        q = qnat[i]
        for c in range(chunks):
            at = pl.ds(c * chunk, chunk)
            dkv[j, 1, at, :] += dot(prob[at, :], dsum_n)
            ds = (score[at, :] * (dot(kv[0, j, 1, at, :], dsum_t) + share)).astype(BF16)
            dsc[at, :] = ds
            dkv[j, 0, at, :] += dot(ds, q) * scale
        dq = dot(kvt[j, 0], dsc[...]) * scale
        qnat[i] = dq.T.astype(BF16)

    def forward(i):
        j = i // 4
        inverse = 1.0 / softmax(1, j, i)
        mix[i] = (dot(kvt[j, 1], prob[...]) * inverse).T.astype(BF16)

    make_kv(0)
    kv_start(0, 0)
    make_q(0)
    make_kv(1)
    make_q(1)
    kv_step(0, 1)
    make_bias()
    for t in range(2, planes - 1):
        kv_step(0, t)
    kv_start(1, 0)
    for n in range(2):
        for k in range(2):
            dkv[n, k] = jnp.zeros((keys, HEAD_DIM), F32)
    for k in range(2):
        for j in range(2):
            kv_copy(0, j, k, planes - 2).wait_recv()
    transposed(0)

    def backward_step(i, _):
        backward(i)

        @pl.when(i < planes - 2)
        def _():
            kv_step(1, i + 1)

        return 0

    lax.fori_loop(0, 8, backward_step, 0)
    for k in range(2):
        for j in range(2):
            kv_copy(1, j, k, planes - 2).wait_recv()
    transposed(1)

    def rs_copy(j, k, t):
        return remote(stage.at[j, k, t], landed.at[j, k, t], rs_send.at[j, k, t], rs_recv.at[j, k, t], to_z[j])

    def rs_step(t, first):
        for k in range(2):
            for j in range(2):
                p = (z + 2 * planes - 1 - t) % planes if j == 0 else (z + 1 + t) % planes
                part = dkv[j, k, pl.ds(pl.multiple_of(p * pair, 32), pair), :]
                if not first:
                    rs_copy(j, k, t - 1).wait_recv()
                    part = part + landed[j, k, t - 1].astype(F32)
                stage[j, k, t] = part.astype(BF16)
                rs_copy(j, k, t).start()

    rs_step(0, True)

    def forward_step(i, _):
        forward(i)

        @pl.when(i < planes - 2)
        def _():
            rs_step(i + 1, False)

        return 0

    lax.fori_loop(0, 8, forward_step, 0)

    mix_swap = to_partner(mix.at[:, theirs, :], mixed.at[pl.ds(8 * h, 8)], 11)
    mix_swap.start()
    for n in range(8):
        mixed[8 * h + n] = mix[n, mine, :]

    def dq_body(i, _):
        d = qnat[i].astype(F32)
        dqkv[i] = (rotated(d, -1.0)).astype(BF16)
        return 0

    lax.fori_loop(0, 8, dq_body, 0)
    dq_all = [jnp.concatenate([dqkv[4 * j + r] for r in range(4)], axis=1) for j in range(2)]

    def dn_q(p, _):
        normed_grad = dot_nt(dq_all[0], wbuf[0, p, :, 0:512]) + dot_nt(dq_all[1], wbuf[1, p, :, 0:512])
        dnown[p] = normed_grad
        return 0

    lax.fori_loop(0, planes, dn_q, 0)

    mix_swap.wait_recv()
    heads_all = jnp.concatenate([mixed[n] for n in range(16)], axis=1)
    for n in range(planes):
        at = pl.ds(n * width, width)
        next_out[:, at] = (xf_in[:, at].astype(F32) + dot(heads_all, wo[:, at])).astype(BF16)

    t = planes - 1
    dkvs = []
    for j in range(2):
        for k in range(2):
            rs_copy(j, k, t - 1).wait_recv()
            part = dkv[j, k, at_z, :] + landed[j, k, t - 1].astype(F32)
            part = part.astype(BF16).astype(F32)
            part = jnp.concatenate([part, jnp.zeros((LANES - pair, HEAD_DIM), F32)], axis=0)
            if k == 0:
                part = rotated(part, -1.0)
            dkvs.append(part.astype(BF16))
    dkv_all = [jnp.concatenate(dkvs[2 * j : 2 * j + 2], axis=1) for j in range(2)]

    def dn_copy(p):
        return remote(dnsend.at[p], dnrecv.at[p], x_send.at[12 + p], x_recv.at[12 + p], partner)

    def dn_kv(p, _):
        dnown[p] += dot_nt(dkv_all[0], wbuf[0, p, :, 512:768]) + dot_nt(dkv_all[1], wbuf[1, p, :, 512:768])
        dnsend[p] = dnown[p, theirs, :].astype(BF16)
        dn_copy(p).start()
        return 0

    lax.fori_loop(0, planes, dn_kv, 0)
    x = xs_in[...].astype(F32)
    inverse = lax.rsqrt(jnp.mean(x * x, axis=-1, keepdims=True) + norm_eps)
    along = jnp.zeros((rows, 1), F32)
    for p in range(planes):
        dn_copy(p).wait_recv()
        at = slice(p * width, (p + 1) * width)
        d = (dnown[p, mine, :] + dnrecv[p].astype(F32)).astype(BF16).astype(F32) * gain_in[:, at]
        dnown[p, mine, :] = d
        along += jnp.sum(d * x[:, at], axis=-1, keepdims=True)
    pull = along * (1.0 / x.shape[1]) * (inverse * inverse * inverse)
    for p in range(planes):
        at = slice(p * width, (p + 1) * width)
        grad = (dnown[p, mine, :] * inverse - x[:, at] * pull).astype(BF16)
        grad_out[:, at] = grad + dy_in[:, at]

    for c in swap:
        c.wait_send()
    mix_swap.wait_send()
    for t in range(planes - 1):
        pos_copy(t).wait_send()
        for j in range(2):
            for c in range(2):
                w_copy(j, t, c).wait_send()
                rs_copy(j, c, t).wait_send()
                for m in range(2):
                    kv_copy(m, j, c, t).wait_send()
    for p in range(planes):
        dn_copy(p).wait_send()


def from_behind(block, axis, distance):
    devices = lax.axis_size(axis)
    route = [((i - distance) % devices, i) for i in range(devices)]
    return lax.ppermute(block, axis, route)


def shards(planes, xf, xs, dy, positions, gain, wq, wkv, wo):
    rows, features = xf.shape[1:]
    keys = 2 * planes * rows
    width = features // planes
    frequency = rope_base ** (-2.0 * jnp.arange(HEAD_DIM // 2, dtype=F32) / HEAD_DIM)
    where = positions.astype(F32)
    angles = where[:, None] * frequency[None, :]
    cos_table, sin_table = jnp.cos(angles), jnp.sin(angles)
    tables = jnp.stack(
        [
            jnp.concatenate([cos_table, cos_table], axis=1),
            jnp.concatenate([-sin_table, sin_table], axis=1),
        ]
    )
    pos_tile = jnp.broadcast_to(jnp.pad(where, (0, 128 - rows))[None, :], (8, 128))
    vmem = pl.BlockSpec(memory_space=pltpu.VMEM)
    hbm = pl.BlockSpec(memory_space=pl.ANY)
    hops = planes - 1
    dma = pltpu.SemaphoreType.DMA
    out = jax.ShapeDtypeStruct((rows, features), BF16)
    produced, grads = pl.pallas_call(
        functools.partial(tick, planes, rows),
        out_shape=(out, out),
        in_specs=[vmem] * 6 + [hbm] * 3,
        out_specs=(vmem, vmem),
        scratch_shapes=[
            pltpu.VMEM((2, planes, width, 768), BF16),
            pltpu.VMEM((features, features), BF16),
            pltpu.VMEM((3, LANES, features), BF16),
            pltpu.VMEM((2, LANES, HEAD_DIM), F32),
            pltpu.VMEM((2 * planes, 8, 128), F32),
            pltpu.VMEM((planes, 2 * LANES, width), BF16),
            pltpu.VMEM((2, 2 * LANES, 768), F32),
            pltpu.VMEM((8, LANES, HEAD_DIM), BF16),
            pltpu.VMEM((2, 8, HEAD_DIM, LANES), BF16),
            pltpu.VMEM((2, 2, 2, keys, HEAD_DIM), BF16),
            pltpu.VMEM((2, 2, HEAD_DIM, keys), BF16),
            pltpu.VMEM((2, 2, keys, HEAD_DIM), F32),
            pltpu.VMEM((keys, LANES), F32),
            pltpu.VMEM((1, LANES), F32),
            pltpu.VMEM((8, HEAD_DIM, LANES), BF16),
            pltpu.VMEM((keys, LANES), F32),
            pltpu.VMEM((keys, LANES), BF16),
            pltpu.VMEM((keys, LANES), BF16),
            pltpu.VMEM((2, 2, hops, 2 * rows, HEAD_DIM), BF16),
            pltpu.VMEM((2, 2, hops, 2 * rows, HEAD_DIM), BF16),
            pltpu.VMEM((8, LANES, HEAD_DIM), BF16),
            pltpu.VMEM((16, rows, HEAD_DIM), BF16),
            pltpu.VMEM((8, LANES, HEAD_DIM), BF16),
            pltpu.VMEM((planes, rows, width), BF16),
            pltpu.VMEM((planes, rows, width), BF16),
            pltpu.VMEM((planes, LANES, width), F32),
            dma((8,)),
            dma((12 + planes,)),
            dma((12 + planes,)),
            dma((2, hops, 2)),
            dma((2, hops, 2)),
            dma((hops,)),
            dma((hops,)),
            dma((2, 2, 2, hops)),
            dma((2, 2, 2, hops)),
            dma((2, 2, hops)),
            dma((2, 2, hops)),
        ],
        compiler_params=pltpu.CompilerParams(
            collective_id=0, has_side_effects=True, vmem_limit_bytes=67_043_328
        ),
        name="tick",
    )(xs[0], xf[0], dy[0], pos_tile, tables, gain, wq[0], wkv[0], wo[0])
    sent_on = from_behind(produced[None], "section", 1)
    sent_back = from_behind(grads[None], "section", -1)
    return sent_on, sent_back


def solution(mesh):
    placed = (
        P("section", "ctx", None),
        P("section", "ctx", None),
        P("section", "ctx", None),
        P("ctx"),
        P("section", None),
        P("section", "ctx", None),
        P("section", "ctx", None),
        P("section", None, None),
    )
    return jax.shard_map(
        functools.partial(shards, mesh.shape["ctx"] // 2),
        mesh=mesh,
        in_specs=placed,
        out_specs=(P("section", "ctx", None), P("section", "ctx", None)),
        check_vma=False,
    )
```

```python
import functools

import jax
import jax.numpy as jnp
from jax import lax
from jax.experimental import pallas as pl
from jax.experimental.pallas import tpu as pltpu
from jax.sharding import PartitionSpec as P

MESH = pl.DeviceIdType.MESH
F32 = jnp.float32
BF16 = jnp.bfloat16
HEAD_DIM = 128
LANES = 256
norm_eps = 1e-05
rope_base = 500000.0
LOG2E = 1.4426950408889634
HIDDEN = -1e30


def dot(a, b):
    return jnp.dot(a, b, preferred_element_type=F32)


def dot_nt(a, b):
    return lax.dot_general(a, b, (((1,), (1,)), ((), ())), preferred_element_type=F32)


def fold_rows(a, op):
    return op(a.reshape(a.shape[0] // 8, 8, a.shape[1]), axis=0)


def tick(
    planes,
    rows,
    xs_in,
    xf_in,
    dy_in,
    pos_in,
    tab_in,
    gain_in,
    wq_hbm,
    wkv_hbm,
    wo_hbm,
    next_out,
    grad_out,
    wkvb,
    wqb,
    wo,
    xbuf,
    tabs,
    posb,
    normed,
    acc_kv,
    acc_q,
    qnat,
    qt,
    kv,
    kvt,
    dkv,
    bias,
    dmt,
    score,
    prob,
    dsc,
    stage,
    landed,
    mix,
    mixed,
    dnsend,
    dnrecv,
    dnown,
    fout,
    gout,
    loc_sem,
    x_send,
    x_recv,
    ring_send,
    ring_recv,
    rs_send,
    rs_recv,
    out_send,
    out_recv,
):
    me = lax.axis_index("ctx")
    section = lax.axis_index("section")
    sections = lax.axis_size("section")
    z = me // 2
    h = me % 2
    partner = z * 2 + 1 - h
    to_z = (((z + 1) % planes) * 2 + h, ((z + planes - 1) % planes) * 2 + h)
    following = (section + 1) % sections
    preceding = (section + sections - 1) % sections
    width = wkvb.shape[1]
    half = width // 2
    pair = 2 * rows
    keys = planes * pair
    chunk = 256
    chunks = keys // chunk
    far = planes // 2
    mine = pl.ds(pl.multiple_of(h * rows, 16), rows)
    theirs = pl.ds(pl.multiple_of((1 - h) * rows, 16), rows)
    scale = HEAD_DIM ** (-0.5)
    scope = jax.named_scope

    barrier = pltpu.get_barrier_semaphore()
    for other in (partner, *to_z):
        pl.semaphore_signal(barrier, inc=1, device_id={"ctx": other}, device_id_type=MESH)
    for other in (following, preceding):
        pl.semaphore_signal(barrier, inc=1, device_id={"section": other}, device_id_type=MESH)

    def local(src, dst, n):
        return pltpu.make_async_copy(src, dst, loc_sem.at[n])

    def remote(src, dst, s, r, **to):
        return pltpu.make_async_remote_copy(
            src_ref=src, dst_ref=dst, send_sem=s, recv_sem=r, device_id=to, device_id_type=MESH
        )

    def to_partner(src, dst, n):
        return remote(src, dst, x_send.at[n], x_recv.at[n], ctx=partner)

    def plane(offset):
        return (z + 2 * planes + offset) % planes

    def pieces(side):
        pairs = []
        for n in range(2):
            at = pl.ds(pl.multiple_of(512 * n + side * 256, 256), 256)
            pairs.append((wkv_hbm.at[:, at], wkvb.at[z, my_rows, pl.ds(256 * n, 256)]))
        for j in range(2):
            at = pl.ds(pl.multiple_of(side * 1024 + j * 512, 512), 512)
            pairs.append((wq_hbm.at[:, at], wqb.at[j, z, my_rows, :]))
        return pairs

    my_rows = pl.ds(pl.multiple_of(h * half, 128), half)
    own = [local(src, dst, n) for n, (src, dst) in enumerate(pieces(h))]
    keep_pos = local(pos_in, posb.at[me], 5)
    for c in (*own, keep_pos):
        c.start()
    load_wo = local(wo_hbm, wo, 4)
    load_wo.start()

    with scope("barrier"):
        pl.semaphore_wait(barrier, 5)

    given = pieces(1 - h)
    tokens = [(src, xbuf.at[n, mine, :]) for n, src in enumerate((xs_in, xf_in, dy_in))]
    swaps = [
        *given[:2],
        (pos_in, posb.at[me]),
        (tab_in, tabs.at[:, mine, :]),
        tokens[0],
        *given[2:],
        *tokens[1:],
    ]
    swap = [to_partner(src, dst, n) for n, (src, dst) in enumerate(swaps)]
    for c in swap:
        c.start()

    class Ring:
        def __init__(self, number, parts):
            self.number, self.parts = number, parts

        def copy(self, n, way, t):
            block = self.parts[n][0](plane(-t if way == 0 else t))
            sems = (self.number, n, way, t)
            return remote(block, block, ring_send.at[sems], ring_recv.at[sems], ctx=to_z[way])

        def step(self, t, ready=None):
            for n, (_, *hops) in enumerate(self.parts):
                if t == 0 and ready is not None:
                    ready(n)
                for way in range(2):
                    if 0 < t <= hops[way]:
                        self.copy(n, way, t - 1).wait_recv()
                    if t < hops[way]:
                        self.copy(n, way, t).start()

        def sent(self):
            for n, (_, *hops) in enumerate(self.parts):
                for way in range(2):
                    for t in range(hops[way]):
                        self.copy(n, way, t).wait_send()

    def rows_of(ref, c):
        who = h if c == 0 else 1 - h
        at = pl.ds(pl.multiple_of(who * half, 128), half)
        return lambda p: ref.at[p, at, :]

    def w_parts(ref):
        return [(rows_of(ref, 0), far, far - 1), (rows_of(ref, 1), far - 1, far)]

    def kv_parts(m):
        def block(j):
            return lambda p: kv.at[m, j, :, pl.ds(pl.multiple_of(p * pair, 32), pair), :]

        return [(block(0), far, far - 1), (block(1), far - 1, far)]

    pos_part = (lambda p: posb.at[pl.ds(2 * p, 2)], far, far - 1)
    ring_wkv = Ring(0, [*w_parts(wkvb), pos_part])
    ring_q = [Ring(1 + j, w_parts(wqb.at[j])) for j in range(2)]
    ring_kv = [Ring(3 + m, kv_parts(m)) for m in range(2)]

    def ready_wkv(n):
        if n == 0:
            own[0].wait()
            own[1].wait()
        elif n == 1:
            swap[0].wait_recv()
            swap[1].wait_recv()
        else:
            keep_pos.wait()
            swap[2].wait_recv()

    def ready_q(j):
        def ready(n):
            if n == 0:
                own[2 + j].wait()
            else:
                swap[5 + j].wait_recv()

        return ready

    def norms(n):
        def body(i, _):
            at = pl.ds(pl.multiple_of(i * 32, 32), 32)
            x = xbuf[n, at, :].astype(F32)
            inverse = lax.rsqrt(jnp.mean(x * x, axis=-1, keepdims=True) + norm_eps)
            y = (x * inverse * gain_in[...]).astype(BF16)
            for p in range(planes):
                normed[p, pl.ds(pl.multiple_of(n * LANES + i * 32, 32), 32), :] = y[:, p * width : (p + 1) * width]
            return 0

        lax.fori_loop(0, LANES // 32, body, 0)

    def project_kv(m):
        at = pl.ds(m * LANES, LANES)
        total = dot(normed[0, at, :], wkvb[0])
        for p in range(1, planes):
            total += dot(normed[p, at, :], wkvb[p])
        acc_kv[...] = total

    def project_q(j, offsets, first=False):
        ps = [plane(o) for o in offsets]
        total = dot(normed[ps[0]], wqb[j, ps[0]])
        for p in ps[1:]:
            total += dot(normed[p], wqb[j, p])
        if first:
            acc_q[j] = total
        else:
            acc_q[j] += total

    def grads_in():
        def body(n, _):
            at = pl.ds(pl.multiple_of(h * 1024 + n * 128, 128), 128)
            dmt[n] = dot_nt(wo[at, :], xbuf[2]).astype(BF16)
            return 0

        lax.fori_loop(0, 8, body, 0)

    def rotated(x, sign):
        return x * tabs[0] + sign * (pltpu.roll(x, HEAD_DIM // 2, 1) * tabs[1])

    at_z = pl.ds(pl.multiple_of(z * pair, 32), pair)

    def make_kv(m):
        for j in range(2):
            key = acc_kv[:, 128 * j : 128 * j + 128]
            kv[m, j, 0, at_z, :] = rotated(key, 1.0).astype(BF16)[:pair]
            kv[m, j, 1, at_z, :] = acc_kv[:, 256 + 128 * j : 384 + 128 * j].astype(BF16)[:pair]

    def make_q(j, m):
        for r in range(4):
            q = rotated(acc_q[j, m * LANES : (m + 1) * LANES, r * 128 : r * 128 + 128], 1.0)
            if m == 0:
                qnat[4 * j + r] = q.astype(BF16)
            qt[m, 4 * j + r] = q.T.astype(BF16)

    def make_bias():
        row0 = posb[2 * z][0:1, :]
        row1 = posb[2 * z + 1][0:1, :]
        zero = jnp.zeros_like(row0)
        wide0 = jnp.concatenate([row0, zero], axis=1)
        wide1 = pltpu.roll(jnp.concatenate([row1, zero], axis=1), rows, 1)
        lane = lax.broadcasted_iota(jnp.int32, (1, LANES), 1)
        query = jnp.where(lane < rows, wide0, jnp.where(lane < pair, wide1, 1e9))

        def body(i, _):
            column = jnp.broadcast_to(posb[i][0:1, :], (128, 128)).T
            column = jnp.concatenate([column, column], axis=1)[:rows]
            at = pl.ds(pl.multiple_of(i * rows, 16), rows)
            bias[at, :] = jnp.where(column <= query, 0.0, HIDDEN)
            return 0

        lax.fori_loop(0, 2 * planes, body, 0)

    def transposed(m, ks):
        for j in range(2):
            for k in ks:
                for i in range(keys // 128):
                    at = pl.ds(i * 128, 128)
                    kvt[j, k, :, at] = kv[m, j, k, at, :].astype(F32).T.astype(BF16)

    def softmax(m, j, i):
        q = qt[m, i]
        top = jnp.full((8, LANES), HIDDEN, F32)
        for c in range(chunks):
            at = pl.ds(c * chunk, chunk)
            s = dot(kv[m, j, 0, at, :], q) + bias[at, :]
            score[at, :] = s
            top = jnp.maximum(top, fold_rows(s, jnp.max))
        top = jnp.max(top, axis=0, keepdims=True)
        total = jnp.zeros((8, LANES), F32)
        for c in range(chunks):
            at = pl.ds(c * chunk, chunk)
            e = jnp.exp2((score[at, :] - top) * (scale * LOG2E))
            total += fold_rows(e, jnp.sum)
            if m == 0:
                score[at, :] = e
            prob[at, :] = e.astype(BF16)
        return jnp.sum(total, axis=0, keepdims=True)

    def backward(j, i):
        inverse = 1.0 / softmax(0, j, i)
        summed = dot(kvt[j, 1], prob[...])
        dm = dmt[i].astype(F32)
        share = -jnp.sum(dm * summed, axis=0, keepdims=True) * (inverse * inverse)
        dsum = dm * inverse
        dsum_t = dsum.astype(BF16)
        dsum_n = dsum.T.astype(BF16)
        q = qnat[i]
        for c in range(chunks):
            at = pl.ds(c * chunk, chunk)
            dkv[j, 1, at, :] += dot(prob[at, :], dsum_n)
            ds = (score[at, :] * (dot(kv[0, j, 1, at, :], dsum_t) + share)).astype(BF16)
            dsc[at, :] = ds
            dkv[j, 0, at, :] += dot(ds, q) * scale
        dq = dot(kvt[j, 0], dsc[...]) * scale
        qnat[i] = dq.T.astype(BF16)

    def forward(j, i):
        inverse = 1.0 / softmax(1, j, i)
        mix[i] = (dot(kvt[j, 1], prob[...]) * inverse).T.astype(BF16)

    rs_hops = ((far - 1, far), (far, far - 1))

    def rs_copy(j, k, way, t):
        at = (j, k, way, t)
        return remote(stage.at[at], landed.at[at], rs_send.at[at], rs_recv.at[at], ctx=to_z[way])

    def rs_step(j, t):
        for k in range(2):
            for way in range(2):
                hops = rs_hops[k][way]
                if 0 < t <= hops:
                    rs_copy(j, k, way, t - 1).wait_recv()
                if t < hops:
                    p = plane(hops - t if way == 0 else t - hops)
                    part = dkv[j, k, pl.ds(pl.multiple_of(p * pair, 32), pair), :]
                    if t > 0:
                        part = part + landed[j, k, way, t - 1].astype(F32)
                    stage[j, k, way, t] = part.astype(BF16)
                    rs_copy(j, k, way, t).start()

    def in_order(i, **steps):
        for name, work in steps.items():
            pl.when(i == int(name[1:]))(work)

    for n in range(3):
        xbuf[n, pl.ds(pair, LANES - pair), :] = jnp.zeros((LANES - pair, xbuf.shape[2]), BF16)
    for n in range(2):
        tabs[n, pl.ds(pair, LANES - pair), :] = jnp.zeros((LANES - pair, HEAD_DIM), F32)
    for n, src in enumerate((xs_in, xf_in, dy_in)):
        xbuf[n, mine, :] = src[...]
    tabs[:, mine, :] = tab_in[...]
    for n in range(2):
        for k in range(2):
            dkv[n, k] = jnp.zeros((keys, HEAD_DIM), F32)

    with scope("a0"):
        ring_wkv.step(0, ready_wkv)
    with scope("a1"):
        ring_wkv.step(1)
    with scope("a2"):
        ring_wkv.step(2)
    with scope("a3"):
        ring_wkv.step(3)
    with scope("c0"):
        ring_q[0].step(0, ready_q(0))
    with scope("norms0"):
        swap[3].wait_recv()
        swap[4].wait_recv()
        norms(0)
    with scope("a4"):
        ring_wkv.step(4)
    with scope("kv0"):
        project_kv(0)
        make_kv(0)
    ring_kv[0].step(0)
    with scope("norms1"):
        swap[7].wait_recv()
        norms(1)
    with scope("c1"):
        ring_q[0].step(1)
    with scope("q0a"):
        project_q(0, (0, 1, -1), True)
    with scope("b1"):
        ring_kv[0].step(1)
    with scope("bias"):
        make_bias()
    with scope("c2"):
        ring_q[0].step(2)
    with scope("q0b"):
        project_q(0, (2, -2))
    with scope("b2"):
        ring_kv[0].step(2)
    with scope("kv1"):
        project_kv(1)
        make_kv(1)
    with scope("c3"):
        ring_q[0].step(3)
    with scope("q0c"):
        project_q(0, (3, -3))
    with scope("b3"):
        ring_kv[0].step(3)
    ring_q[1].step(0, ready_q(1))
    with scope("dm"):
        load_wo.wait()
        swap[8].wait_recv()
        grads_in()
    with scope("c4"):
        ring_q[0].step(4)
    with scope("q0d"):
        project_q(0, (4,))
        make_q(0, 0)
    with scope("b4"):
        ring_kv[0].step(4)
    with scope("t0"):
        transposed(0, (0, 1))
    with scope("d1"):
        ring_q[1].step(1)

    def backward0(i, _):
        with scope("bwd"):
            backward(0, i)

        def first():
            with scope("d2"):
                ring_q[1].step(2)

        def second():
            with scope("d3"):
                ring_q[1].step(3)
            ring_kv[1].step(0)

        in_order(i, i1=first, i3=second)
        return 0

    lax.fori_loop(0, 4, backward0, 0)
    rs_step(0, 0)
    with scope("q1a"):
        project_q(1, (0, 1, -1, 2, -2, 3, -3), True)
        make_q(0, 1)
    with scope("d4"):
        ring_q[1].step(4)
    with scope("q1b"):
        project_q(1, (4,))
        make_q(1, 0)

    def backward1(i, _):
        with scope("bwd"):
            backward(1, 4 + i)

        def g(t):
            def work():
                with scope("g"):
                    rs_step(0, t)

            return work

        def last():
            g(3)()
            with scope("f1"):
                ring_kv[1].step(1)

        in_order(i, i0=g(1), i1=g(2), i2=last)
        return 0

    lax.fori_loop(0, 4, backward1, 0)
    rs_step(1, 0)
    with scope("g4"):
        rs_step(0, 4)
    make_q(1, 1)
    with scope("f2"):
        ring_kv[1].step(2)
    with scope("g1"):
        rs_step(1, 1)
    with scope("f3"):
        ring_kv[1].step(3)
    with scope("g2"):
        rs_step(1, 2)
    with scope("f4"):
        ring_kv[1].step(4)
    with scope("t1"):
        transposed(1, (1,))
    with scope("g3"):
        rs_step(1, 3)

    for j in range(2):
        def forward_step(i, _):
            with scope("fwd"):
                forward(j, 4 * j + i)
            return 0

        lax.fori_loop(0, 4, forward_step, 0)

    mix_swap = to_partner(mix.at[:, theirs, :], mixed.at[pl.ds(8 * h, 8)], 9)
    mix_swap.start()

    def dn_copy(p):
        return to_partner(dnsend.at[p], dnrecv.at[p], 10 + p)

    def unrotated(x):
        return rotated(x, -1.0).astype(BF16)

    with scope("dq"):
        dq_all = [
            jnp.concatenate([unrotated(qnat[4 * j + r].astype(F32)) for r in range(4)], axis=1) for j in range(2)
        ]
    with scope("g4"):
        rs_step(1, 4)
    with scope("dkv"):
        parts = []
        for k in range(2):
            for j in range(2):
                part = dkv[j, k, at_z, :]
                for way in range(2):
                    part = part + landed[j, k, way, rs_hops[k][way] - 1].astype(F32)
                part = part.astype(BF16).astype(F32)
                part = jnp.concatenate([part, jnp.zeros((LANES - pair, HEAD_DIM), F32)], axis=0)
                parts.append(unrotated(part) if k == 0 else part.astype(BF16))
        dkv_all = jnp.concatenate(parts, axis=1)

    def dn_step(p, _):
        dnown[p] = dot_nt(dq_all[0], wqb[0, p]) + dot_nt(dq_all[1], wqb[1, p]) + dot_nt(dkv_all, wkvb[p])
        dnsend[p] = dnown[p, theirs, :].astype(BF16)
        dn_copy(p).start()
        return 0

    with scope("dn"):
        lax.fori_loop(0, planes, dn_step, 0)

    def out_copy(which, p):
        at = pl.ds(p * width, width)
        src, dst, to = ((fout, next_out, following), (gout, grad_out, preceding))[which]
        return remote(
            src.at[:, at], dst.at[:, at], out_send.at[which, p], out_recv.at[which, p], section=to
        )

    with scope("out"):
        for n in range(8):
            mixed[8 * h + n] = mix[n, mine, :]
        mix_swap.wait_recv()
        heads_all = jnp.concatenate([mixed[n] for n in range(16)], axis=1)
        for n in range(planes):
            at = pl.ds(n * width, width)
            fout[:, at] = (xf_in[:, at].astype(F32) + dot(heads_all, wo[:, at])).astype(BF16)
            out_copy(0, n).start()

    x = xs_in[...].astype(F32)
    inverse = lax.rsqrt(jnp.mean(x * x, axis=-1, keepdims=True) + norm_eps)
    along = jnp.zeros((rows, 1), F32)
    with scope("dnwait"):
        for p in range(planes):
            dn_copy(p).wait_recv()
            at = slice(p * width, (p + 1) * width)
            d = (dnown[p, mine, :] + dnrecv[p].astype(F32)).astype(BF16).astype(F32) * gain_in[:, at]
            dnown[p, mine, :] = d
            along += jnp.sum(d * x[:, at], axis=-1, keepdims=True)
    pull = along * (1.0 / x.shape[1]) * (inverse * inverse * inverse)
    with scope("grad"):
        for p in range(planes):
            at = slice(p * width, (p + 1) * width)
            grad = (dnown[p, mine, :] * inverse - x[:, at] * pull).astype(BF16)
            gout[:, at] = grad + dy_in[:, at]
            out_copy(1, p).start()

    with scope("sent"):
        for c in (*swap, mix_swap):
            c.wait_send()
        for ring in (ring_wkv, *ring_q, *ring_kv):
            ring.sent()
        for j in range(2):
            for k in range(2):
                for way in range(2):
                    for t in range(rs_hops[k][way]):
                        rs_copy(j, k, way, t).wait_send()
        for p in range(planes):
            dn_copy(p).wait_send()
    with scope("outs"):
        for which in range(2):
            for p in range(planes):
                out_copy(which, p).wait()


def shards(planes, xf, xs, dy, positions, gain, wq, wkv, wo):
    rows, features = xf.shape[1:]
    keys = 2 * planes * rows
    width = features // planes
    frequency = rope_base ** (-2.0 * jnp.arange(HEAD_DIM // 2, dtype=F32) / HEAD_DIM)
    where = positions.astype(F32)
    angles = where[:, None] * frequency[None, :]
    cos_table, sin_table = jnp.cos(angles), jnp.sin(angles)
    tables = jnp.stack(
        [
            jnp.concatenate([cos_table, cos_table], axis=1),
            jnp.concatenate([-sin_table, sin_table], axis=1),
        ]
    )
    pos_tile = jnp.broadcast_to(jnp.pad(where, (0, 128 - rows))[None, :], (8, 128))
    vmem = pl.BlockSpec(memory_space=pltpu.VMEM)
    hbm = pl.BlockSpec(memory_space=pl.ANY)
    far = planes // 2
    dma = pltpu.SemaphoreType.DMA
    out = jax.ShapeDtypeStruct((rows, features), BF16)
    produced, grads = pl.pallas_call(
        functools.partial(tick, planes, rows),
        out_shape=(out, out),
        in_specs=[vmem] * 6 + [hbm] * 3,
        out_specs=(vmem, vmem),
        scratch_shapes=[
            pltpu.VMEM((planes, width, 512), BF16),
            pltpu.VMEM((2, planes, width, 512), BF16),
            pltpu.VMEM((features, features), BF16),
            pltpu.VMEM((3, LANES, features), BF16),
            pltpu.VMEM((2, LANES, HEAD_DIM), F32),
            pltpu.VMEM((2 * planes, 8, 128), F32),
            pltpu.VMEM((planes, 2 * LANES, width), BF16),
            pltpu.VMEM((LANES, 512), F32),
            pltpu.VMEM((2, 2 * LANES, 512), F32),
            pltpu.VMEM((8, LANES, HEAD_DIM), BF16),
            pltpu.VMEM((2, 8, HEAD_DIM, LANES), BF16),
            pltpu.VMEM((2, 2, 2, keys, HEAD_DIM), BF16),
            pltpu.VMEM((2, 2, HEAD_DIM, keys), BF16),
            pltpu.VMEM((2, 2, keys, HEAD_DIM), F32),
            pltpu.VMEM((keys, LANES), F32),
            pltpu.VMEM((8, HEAD_DIM, LANES), BF16),
            pltpu.VMEM((keys, LANES), F32),
            pltpu.VMEM((keys, LANES), BF16),
            pltpu.VMEM((keys, LANES), BF16),
            pltpu.VMEM((2, 2, 2, far, 2 * rows, HEAD_DIM), BF16),
            pltpu.VMEM((2, 2, 2, far, 2 * rows, HEAD_DIM), BF16),
            pltpu.VMEM((8, LANES, HEAD_DIM), BF16),
            pltpu.VMEM((16, rows, HEAD_DIM), BF16),
            pltpu.VMEM((planes, rows, width), BF16),
            pltpu.VMEM((planes, rows, width), BF16),
            pltpu.VMEM((planes, LANES, width), F32),
            pltpu.VMEM((rows, features), BF16),
            pltpu.VMEM((rows, features), BF16),
            dma((6,)),
            dma((10 + planes,)),
            dma((10 + planes,)),
            dma((5, 3, 2, far)),
            dma((5, 3, 2, far)),
            dma((2, 2, 2, far)),
            dma((2, 2, 2, far)),
            dma((2, planes)),
            dma((2, planes)),
        ],
        compiler_params=pltpu.CompilerParams(
            collective_id=0, has_side_effects=True, vmem_limit_bytes=67_043_328
        ),
        name="tick",
    )(xs[0], xf[0], dy[0], pos_tile, tables, gain, wq[0], wkv[0], wo[0])
    return produced[None], grads[None]


def solution(mesh):
    placed = (
        P("section", "ctx", None),
        P("section", "ctx", None),
        P("section", "ctx", None),
        P("ctx"),
        P("section", None),
        P("section", "ctx", None),
        P("section", "ctx", None),
        P("section", None, None),
    )
    return jax.shard_map(
        functools.partial(shards, mesh.shape["ctx"] // 2),
        mesh=mesh,
        in_specs=placed,
        out_specs=(P("section", "ctx", None), P("section", "ctx", None)),
        check_vma=False,
    )
```

```python
import functools

import jax
import jax.numpy as jnp
from jax import lax
from jax.experimental import pallas as pl
from jax.experimental.pallas import tpu as pltpu
from jax.sharding import PartitionSpec as P

MESH = pl.DeviceIdType.MESH
F32 = jnp.float32
BF16 = jnp.bfloat16
HEAD_DIM = 128
LANES = 256
norm_eps = 1e-05
rope_base = 500000.0
LOG2E = 1.4426950408889634
HIDDEN = -1e30


def dot(a, b):
    return jnp.dot(a, b, preferred_element_type=F32)


def dot_nt(a, b):
    return lax.dot_general(a, b, (((1,), (1,)), ((), ())), preferred_element_type=F32)


def fold_rows(a, op):
    return op(a.reshape(a.shape[0] // 8, 8, a.shape[1]), axis=0)


def tick(
    planes,
    rows,
    xs_in,
    xf_in,
    dy_in,
    pos_in,
    tab_in,
    gain_in,
    wq_hbm,
    wkv_hbm,
    wo_hbm,
    next_out,
    grad_out,
    wkvb,
    wqb,
    wo,
    xbuf,
    tabs,
    posb,
    normed,
    acc_kv,
    acc_q,
    qnat,
    qt,
    kv,
    kvt,
    dkv,
    bias,
    dmt,
    score,
    prob,
    dsc,
    stage,
    landed,
    mix,
    mixed,
    dnsend,
    dnrecv,
    dnown,
    fout,
    gout,
    wlent,
    last,
    lastrecv,
    passing,
    loc_sem,
    x_send,
    x_recv,
    ring_send,
    ring_recv,
    rs_send,
    rs_recv,
    mix_send,
    mix_recv,
    out_send,
    out_recv,
    relay_send,
    relay_recv,
):
    me = lax.axis_index("ctx")
    section = lax.axis_index("section")
    sections = lax.axis_size("section")
    z = me // 2
    h = me % 2
    partner = z * 2 + 1 - h
    to_z = (((z + 1) % planes) * 2 + h, ((z + planes - 1) % planes) * 2 + h)
    following = (section + 1) % sections
    preceding = (section + sections - 1) % sections
    width = wkvb.shape[1]
    half = width // 2
    pair = 2 * rows
    keys = planes * pair
    chunk = 256
    chunks = keys // chunk
    far = planes // 2
    mine = pl.ds(pl.multiple_of(h * rows, 16), rows)
    theirs = pl.ds(pl.multiple_of((1 - h) * rows, 16), rows)
    scale = HEAD_DIM ** (-0.5)
    scope = jax.named_scope

    barrier = pltpu.get_barrier_semaphore()
    for other in (partner, *to_z):
        pl.semaphore_signal(barrier, inc=1, device_id={"ctx": other}, device_id_type=MESH)
    for other in (following, preceding):
        pl.semaphore_signal(barrier, inc=1, device_id={"section": other}, device_id_type=MESH)

    relayed = sections > 1
    core = section % 2
    x_hi = (section // 2) % 2
    base = section - section % 4

    def x_down(hi):
        return h * hi + (1 - h) * (1 - hi)

    def x_up(hi):
        return (1 - h) * hi + h * (1 - hi)

    relay = base + 2 * x_down(x_hi)
    source = base + 2 * x_up(x_hi)
    end = (source + sections - 1) % sections
    ahead = following - following % 4 + 2 * x_down((following // 2) % 2)

    def greet(to):
        pl.semaphore_signal(
            barrier, inc=1, device_id={"section": to, "ctx": partner}, device_id_type=MESH
        )

    if relayed:

        @pl.when(core == 0)
        def _():
            for to in (relay, source, end):
                greet(to)

        @pl.when(core == 1)
        def _():
            greet(ahead)

    def local(src, dst, n):
        return pltpu.make_async_copy(src, dst, loc_sem.at[n])

    def remote(src, dst, s, r, **to):
        return pltpu.make_async_remote_copy(
            src_ref=src, dst_ref=dst, send_sem=s, recv_sem=r, device_id=to, device_id_type=MESH
        )

    def to_partner(src, dst, n):
        return remote(src, dst, x_send.at[n], x_recv.at[n], ctx=partner)

    def plane(offset):
        return (z + 2 * planes + offset) % planes

    def pieces(side):
        pairs = []
        for n in range(2):
            at = pl.ds(pl.multiple_of(512 * n + side * 256, 256), 256)
            pairs.append((wkv_hbm.at[:, at], wkvb.at[z, my_rows, pl.ds(256 * n, 256)]))
        for j in range(2):
            at = pl.ds(pl.multiple_of(side * 1024 + j * 512, 512), 512)
            pairs.append((wq_hbm.at[:, at], wqb.at[j, z, my_rows, :]))
        return pairs

    my_rows = pl.ds(pl.multiple_of(h * half, 128), half)
    own = [local(src, dst, n) for n, (src, dst) in enumerate(pieces(h))]
    keep_pos = local(pos_in, posb.at[me], 5)
    for c in (*own, keep_pos):
        c.start()
    load_wo = local(wo_hbm, wo, 4)
    load_wo.start()

    for n in range(3):
        xbuf[n, pl.ds(pair, LANES - pair), :] = jnp.zeros((LANES - pair, xbuf.shape[2]), BF16)
    for n in range(2):
        tabs[n, pl.ds(pair, LANES - pair), :] = jnp.zeros((LANES - pair, HEAD_DIM), F32)
    for n, src in enumerate((xs_in, xf_in, dy_in)):
        xbuf[n, mine, :] = src[...]
    tabs[:, mine, :] = tab_in[...]
    for n in range(2):
        for k in range(2):
            dkv[n, k] = jnp.zeros((keys, HEAD_DIM), F32)

    with scope("barrier"):
        if relayed:
            pl.when(core == 0)(lambda: pl.semaphore_wait(barrier, 8))
            pl.when(core == 1)(lambda: pl.semaphore_wait(barrier, 6))
        else:
            pl.semaphore_wait(barrier, 5)

    given = pieces(1 - h)
    tokens = [(src, xbuf.at[n, mine, :]) for n, src in enumerate((xs_in, xf_in, dy_in))]
    swaps = [
        *given[:2],
        (pos_in, posb.at[me]),
        (tab_in, tabs.at[:, mine, :]),
        tokens[0],
        *given[2:],
        *tokens[1:],
    ]
    swap = [to_partner(src, dst, n) for n, (src, dst) in enumerate(swaps)]
    for c in swap:
        c.start()

    class Ring:
        def __init__(self, number, parts):
            self.number, self.parts = number, parts

        def copy(self, n, way, t):
            block = self.parts[n][0](plane(-t if way == 0 else t))
            sems = (self.number, n, way, t)
            return remote(block, block, ring_send.at[sems], ring_recv.at[sems], ctx=to_z[way])

        def step(self, t, ready=None, only=None):
            for n, (_, *hops) in enumerate(self.parts):
                if only is not None and n != only:
                    continue
                if t == 0 and ready is not None:
                    ready(n)
                for way in range(2):
                    if 0 < t <= hops[way]:
                        self.copy(n, way, t - 1).wait_recv()
                    if t < hops[way]:
                        self.copy(n, way, t).start()

        def sent(self):
            for n, (_, *hops) in enumerate(self.parts):
                for way in range(2):
                    for t in range(hops[way]):
                        self.copy(n, way, t).wait_send()

    def rows_of(ref, c):
        who = h if c == 0 else 1 - h
        at = pl.ds(pl.multiple_of(who * half, 128), half)
        return lambda p: ref.at[p, at, :]

    def w_parts(ref):
        return [(rows_of(ref, 0), far, far - 1), (rows_of(ref, 1), far - 1, far)]

    def kv_parts(m):
        def block(j):
            return lambda p: kv.at[m, j, :, pl.ds(pl.multiple_of(p * pair, 32), pair), :]

        return [(block(0), far, far - 1), (block(1), far - 1, far)]

    pos_part = (lambda p: posb.at[pl.ds(2 * p, 2)], far, far - 1)
    ring_wkv = Ring(0, [*w_parts(wkvb), pos_part])
    ring_q = [Ring(1 + j, w_parts(wqb.at[j])) for j in range(2)]
    ring_kv = [Ring(3 + m, kv_parts(m)) for m in range(2)]

    def ready_wkv(n):
        if n == 0:
            own[0].wait()
            own[1].wait()
        elif n == 1:
            swap[0].wait_recv()
            swap[1].wait_recv()
        else:
            keep_pos.wait()
            swap[2].wait_recv()

    def ready_q(j):
        def ready(n):
            if n == 0:
                own[2 + j].wait()
            else:
                swap[5 + j].wait_recv()

        return ready

    def norms(n):
        def body(i, _):
            at = pl.ds(pl.multiple_of(i * 32, 32), 32)
            x = xbuf[n, at, :].astype(F32)
            inverse = lax.rsqrt(jnp.mean(x * x, axis=-1, keepdims=True) + norm_eps)
            y = (x * inverse * gain_in[...]).astype(BF16)
            for p in range(planes):
                normed[p, pl.ds(pl.multiple_of(n * LANES + i * 32, 32), 32), :] = y[:, p * width : (p + 1) * width]
            return 0

        lax.fori_loop(0, LANES // 32, body, 0)

    def project_kv(m):
        at = pl.ds(m * LANES, LANES)
        total = dot(normed[0, at, :], wkvb[0])
        for p in range(1, planes):
            total += dot(normed[p, at, :], wkvb[p])
        acc_kv[...] = total

    def project_q(j, offsets, first=False):
        ps = [plane(o) for o in offsets]
        total = dot(normed[ps[0]], wqb[j, ps[0]])
        for p in ps[1:]:
            total += dot(normed[p], wqb[j, p])
        if first:
            acc_q[j] = total
        else:
            acc_q[j] += total

    def grads_in():
        def body(n, _):
            at = pl.ds(pl.multiple_of(h * 1024 + n * 128, 128), 128)
            dmt[n] = dot_nt(wo[at, :], xbuf[2]).astype(BF16)
            return 0

        lax.fori_loop(0, 8, body, 0)

    def rotated(x, sign):
        return x * tabs[0] + sign * (pltpu.roll(x, HEAD_DIM // 2, 1) * tabs[1])

    at_z = pl.ds(pl.multiple_of(z * pair, 32), pair)

    def make_kv(m):
        for j in range(2):
            key = acc_kv[:, 128 * j : 128 * j + 128]
            kv[m, j, 0, at_z, :] = rotated(key, 1.0).astype(BF16)[:pair]
            kv[m, j, 1, at_z, :] = acc_kv[:, 256 + 128 * j : 384 + 128 * j].astype(BF16)[:pair]

    def make_q(j, m):
        for r in range(4):
            q = rotated(acc_q[j, m * LANES : (m + 1) * LANES, r * 128 : r * 128 + 128], 1.0)
            if m == 0:
                qnat[4 * j + r] = q.astype(BF16)
            qt[m, 4 * j + r] = q.T.astype(BF16)

    def make_bias():
        row0 = posb[2 * z][0:1, :]
        row1 = posb[2 * z + 1][0:1, :]
        zero = jnp.zeros_like(row0)
        wide0 = jnp.concatenate([row0, zero], axis=1)
        wide1 = pltpu.roll(jnp.concatenate([row1, zero], axis=1), rows, 1)
        lane = lax.broadcasted_iota(jnp.int32, (1, LANES), 1)
        query = jnp.where(lane < rows, wide0, jnp.where(lane < pair, wide1, 1e9))

        def body(i, _):
            column = jnp.broadcast_to(posb[i][0:1, :], (128, 128)).T
            column = jnp.concatenate([column, column], axis=1)[:rows]
            at = pl.ds(pl.multiple_of(i * rows, 16), rows)
            bias[at, :] = jnp.where(column <= query, 0.0, HIDDEN)
            return 0

        lax.fori_loop(0, 2 * planes, body, 0)

    def transposed(m, ks):
        for j in range(2):
            for k in ks:
                for i in range(keys // 128):
                    at = pl.ds(i * 128, 128)
                    kvt[j, k, :, at] = kv[m, j, k, at, :].astype(F32).T.astype(BF16)

    def softmax(m, j, i):
        q = qt[m, i]
        top = jnp.full((8, LANES), HIDDEN, F32)
        for c in range(chunks):
            at = pl.ds(c * chunk, chunk)
            s = dot(kv[m, j, 0, at, :], q) + bias[at, :]
            score[at, :] = s
            top = jnp.maximum(top, fold_rows(s, jnp.max))
        top = jnp.max(top, axis=0, keepdims=True)
        total = jnp.zeros((8, LANES), F32)
        for c in range(chunks):
            at = pl.ds(c * chunk, chunk)
            e = jnp.exp2((score[at, :] - top) * (scale * LOG2E))
            total += fold_rows(e, jnp.sum)
            if m == 0:
                score[at, :] = e
            prob[at, :] = e.astype(BF16)
        return jnp.sum(total, axis=0, keepdims=True)

    def backward(j, i):
        inverse = 1.0 / softmax(0, j, i)
        summed = dot(kvt[j, 1], prob[...])
        dm = dmt[i].astype(F32)
        share = -jnp.sum(dm * summed, axis=0, keepdims=True) * (inverse * inverse)
        dsum = dm * inverse
        dsum_t = dsum.astype(BF16)
        dsum_n = dsum.T.astype(BF16)
        q = qnat[i]
        for c in range(chunks):
            at = pl.ds(c * chunk, chunk)
            dkv[j, 1, at, :] += dot(prob[at, :], dsum_n)
            ds = (score[at, :] * (dot(kv[0, j, 1, at, :], dsum_t) + share)).astype(BF16)
            dsc[at, :] = ds
            dkv[j, 0, at, :] += dot(ds, q) * scale
        dq = dot(kvt[j, 0], dsc[...]) * scale
        qnat[i] = dq.T.astype(BF16)

    def forward(j, i):
        inverse = 1.0 / softmax(1, j, i)
        mix[i] = (dot(kvt[j, 1], prob[...]) * inverse).T.astype(BF16)

    rs_hops = ((far - 1, far), (far, far - 1))

    def rs_copy(j, k, way, t):
        at = (j, k, way, t)
        return remote(stage.at[at], landed.at[at], rs_send.at[at], rs_recv.at[at], ctx=to_z[way])

    def rs_step(j, t):
        for k in range(2):
            for way in range(2):
                hops = rs_hops[k][way]
                if 0 < t <= hops:
                    rs_copy(j, k, way, t - 1).wait_recv()
                if t < hops:
                    p = plane(hops - t if way == 0 else t - hops)
                    part = dkv[j, k, pl.ds(pl.multiple_of(p * pair, 32), pair), :]
                    if t > 0:
                        part = part + landed[j, k, way, t - 1].astype(F32)
                    stage[j, k, way, t] = part.astype(BF16)
                    rs_copy(j, k, way, t).start()

    def in_order(i, **steps):
        for name, work in steps.items():
            pl.when(i == int(name[1:]))(work)

    def lend(k):
        at = pl.ds(256 * k + 128, 128)
        return to_partner(wkvb.at[:, :, at], wlent.at[:, :, pl.ds(128 * k, 128)], 10 + k)

    with scope("a0"):
        ring_wkv.step(0, ready_wkv, 0)
        ring_q[0].step(0, ready_q(0), 0)
        ring_wkv.step(0, ready_wkv, 1)
        ring_wkv.step(0, ready_wkv, 2)
    with scope("a1"):
        ring_wkv.step(1)
    with scope("a2"):
        ring_wkv.step(2)
    with scope("a3"):
        ring_wkv.step(3)
    with scope("c0"):
        ring_q[0].step(0, ready_q(0), 1)
    with scope("norms0"):
        swap[3].wait_recv()
        swap[4].wait_recv()
        norms(0)
    with scope("a4"):
        ring_wkv.step(4)
    for k in range(2):
        lend(k).start()
    with scope("kv0"):
        project_kv(0)
        make_kv(0)
    ring_kv[0].step(0)
    with scope("c1"):
        ring_q[0].step(1)
    with scope("b1"):
        ring_kv[0].step(1)
    with scope("bias"):
        make_bias()
    with scope("c2"):
        ring_q[0].step(2)
    with scope("b2"):
        ring_kv[0].step(2)
    with scope("norms1"):
        swap[7].wait_recv()
        norms(1)
    with scope("kv1"):
        project_kv(1)
        make_kv(1)
    with scope("c3"):
        ring_q[0].step(3)
    with scope("q0c"):
        project_q(0, (0, 1, -1, 2, -2, 3, -3), True)
    with scope("b3"):
        ring_kv[0].step(3)
    ring_q[1].step(0, ready_q(1))
    with scope("dm"):
        load_wo.wait()
        swap[8].wait_recv()
        grads_in()
    with scope("c4"):
        ring_q[0].step(4)
    with scope("q0d"):
        project_q(0, (4,))
        make_q(0, 0)
    with scope("b4"):
        ring_kv[0].step(4)
    with scope("t0"):
        transposed(0, (0, 1))

    def backward0(i, _):
        with scope("bwd"):
            backward(0, i)

        def d(t):
            def work():
                with scope("d"):
                    ring_q[1].step(t)
                    if t == 3:
                        ring_kv[1].step(0)

            return work

        in_order(i, i0=d(1), i2=d(2), i3=d(3))
        return 0

    lax.fori_loop(0, 4, backward0, 0)
    rs_step(0, 0)
    with scope("q1a"):
        project_q(1, (0, 1, -1, 2, -2, 3, -3), True)
        make_q(0, 1)
    with scope("d4"):
        ring_q[1].step(4)
    with scope("q1b"):
        project_q(1, (4,))
        make_q(1, 0)

    def backward1(i, _):
        with scope("bwd"):
            backward(1, 4 + i)

        def g(t):
            def work():
                with scope("g"):
                    rs_step(0, t)
                with scope("f"):
                    ring_kv[1].step(t)

            return work

        in_order(i, i0=g(1), i1=g(2), i2=g(3))
        return 0

    lax.fori_loop(0, 4, backward1, 0)
    rs_step(1, 0)
    with scope("g4"):
        rs_step(0, 4)

    def unrotated(x):
        return rotated(x, -1.0).astype(BF16)

    def owned(j):
        parts = []
        for k in range(2):
            part = dkv[j, k, at_z, :]
            for way in range(2):
                part = part + landed[j, k, way, rs_hops[k][way] - 1].astype(F32)
            part = part.astype(BF16).astype(F32)
            part = jnp.concatenate([part, jnp.zeros((LANES - pair, HEAD_DIM), F32)], axis=0)
            parts.append(unrotated(part) if k == 0 else part.astype(BF16))
        return jnp.concatenate(parts, axis=1)

    def dn_copy(p):
        return to_partner(dnsend.at[p], dnrecv.at[p], 14 + p)

    with scope("dq"):
        dq_all = [
            jnp.concatenate([unrotated(qnat[4 * j + r].astype(F32)) for r in range(4)], axis=1) for j in range(2)
        ]
        dkv0 = owned(0)

    def first_w(p):
        return jnp.concatenate([wkvb[p, :, 0:128], wkvb[p, :, 256:384]], axis=1)

    def second_w(p):
        return jnp.concatenate([wkvb[p, :, 128:256], wkvb[p, :, 384:512]], axis=1)

    def dn_step(p, _):
        dnown[p] = dot_nt(dq_all[0], wqb[0, p]) + dot_nt(dq_all[1], wqb[1, p]) + dot_nt(dkv0, first_w(p))
        dnsend[p] = dnown[p, theirs, :].astype(BF16)
        dn_copy(p).start()
        return 0

    with scope("dn"):
        lax.fori_loop(0, planes, dn_step, 0)
    with scope("f4"):
        ring_kv[1].step(4)
    with scope("t1"):
        transposed(1, (1,))
        make_q(1, 1)

    def mix_copy(i):
        return remote(
            mix.at[i, theirs, :], mixed.at[8 * h + i], mix_send.at[i], mix_recv.at[i], ctx=partner
        )

    def forward_step(i, _):
        with scope("fwd"):
            forward(i // 4, i)
        mix_copy(i).start()

        def g(t):
            def work():
                with scope("g"):
                    rs_step(1, t)

            return work

        in_order(i, i1=g(1), i4=g(2), i6=g(3))
        return 0

    lax.fori_loop(0, 8, forward_step, 0)

    with scope("g4"):
        rs_step(1, 4)
    with scope("dkv"):
        last[...] = owned(1)
    last_swap = to_partner(last.at[theirs, :], lastrecv, 12)
    last_swap.start()

    def out_copy(which, p):
        at = pl.ds(p * width, width)
        src, dst, to = ((fout, next_out, following), (gout, grad_out, preceding))[which]
        return remote(
            src.at[:, at], dst.at[:, at], out_send.at[which, p], out_recv.at[which, p], section=to
        )

    by_relay = (0, 2, 4, 6)

    def relay_in(p):
        at = pl.ds(p * width, width)
        return remote(
            gout.at[:, at], passing.at[p], out_send.at[1, p], relay_recv.at[p], section=relay, ctx=partner
        )

    def relay_out(p):
        at = pl.ds(p * width, width)
        return remote(
            passing.at[p], grad_out.at[:, at], relay_send.at[p], out_recv.at[1, p], section=end, ctx=partner
        )

    def send_grad(p):
        if relayed and p in by_relay:
            pl.when(core == 0)(lambda: relay_in(p).start())
            pl.when(core == 1)(lambda: out_copy(1, p).start())
        else:
            out_copy(1, p).start()

    with scope("out"):
        for n in range(8):
            mixed[8 * h + n] = mix[n, mine, :]
        for n in range(8):
            mix_copy(n).wait_recv()
        heads_all = jnp.concatenate([mixed[n] for n in range(16)], axis=1)
        for n in range(planes):
            at = pl.ds(n * width, width)
            fout[:, at] = (xf_in[:, at].astype(F32) + dot(heads_all, wo[:, at])).astype(BF16)
            out_copy(0, n).start()

    x = xs_in[...].astype(F32)
    inverse = lax.rsqrt(jnp.mean(x * x, axis=-1, keepdims=True) + norm_eps)
    along = jnp.zeros((rows, 1), F32)
    with scope("dnwait"):
        for p in range(planes):
            dn_copy(p).wait_recv()
        for k in range(2):
            lend(k).wait_recv()
        last_swap.wait_recv()
    with scope("last"):
        own_last = last[mine, :]
        for p in range(planes):
            at = slice(p * width, (p + 1) * width)
            total = dnown[p, mine, :] + dnrecv[p].astype(F32)
            total += dot_nt(own_last, second_w(p)) + dot_nt(lastrecv[...], wlent[p])
            d = total.astype(BF16).astype(F32) * gain_in[:, at]
            dnown[p, mine, :] = d
            along += jnp.sum(d * x[:, at], axis=-1, keepdims=True)
    pull = along * (1.0 / x.shape[1]) * (inverse * inverse * inverse)
    with scope("grad"):
        for p in range(planes):
            at = slice(p * width, (p + 1) * width)
            grad = (dnown[p, mine, :] * inverse - x[:, at] * pull).astype(BF16)
            gout[:, at] = grad + dy_in[:, at]
            send_grad(p)

    if relayed:

        @pl.when(core == 0)
        def _():
            with scope("relay"):
                for p in by_relay:
                    relay_in(p).wait_recv()
                    relay_out(p).start()

    with scope("sent"):
        for c in (*swap, last_swap, lend(0), lend(1), *(mix_copy(n) for n in range(8))):
            c.wait_send()
        for ring in (ring_wkv, *ring_q, *ring_kv):
            ring.sent()
        for j in range(2):
            for k in range(2):
                for way in range(2):
                    for t in range(rs_hops[k][way]):
                        rs_copy(j, k, way, t).wait_send()
        for p in range(planes):
            dn_copy(p).wait_send()
    with scope("outs"):
        for which in range(2):
            for p in range(planes):
                out_copy(which, p).wait()
        if relayed:

            @pl.when(core == 0)
            def _():
                for p in by_relay:
                    relay_out(p).wait_send()


def shards(planes, xf, xs, dy, positions, gain, wq, wkv, wo):
    rows, features = xf.shape[1:]
    keys = 2 * planes * rows
    width = features // planes
    frequency = rope_base ** (-2.0 * jnp.arange(HEAD_DIM // 2, dtype=F32) / HEAD_DIM)
    where = positions.astype(F32)
    angles = where[:, None] * frequency[None, :]
    cos_table, sin_table = jnp.cos(angles), jnp.sin(angles)
    tables = jnp.stack(
        [
            jnp.concatenate([cos_table, cos_table], axis=1),
            jnp.concatenate([-sin_table, sin_table], axis=1),
        ]
    )
    pos_tile = jnp.broadcast_to(jnp.pad(where, (0, 128 - rows))[None, :], (8, 128))
    vmem = pl.BlockSpec(memory_space=pltpu.VMEM)
    hbm = pl.BlockSpec(memory_space=pl.ANY)
    far = planes // 2
    dma = pltpu.SemaphoreType.DMA
    out = jax.ShapeDtypeStruct((rows, features), BF16)
    produced, grads = pl.pallas_call(
        functools.partial(tick, planes, rows),
        out_shape=(out, out),
        in_specs=[vmem] * 6 + [hbm] * 3,
        out_specs=(vmem, vmem),
        scratch_shapes=[
            pltpu.VMEM((planes, width, 512), BF16),
            pltpu.VMEM((2, planes, width, 512), BF16),
            pltpu.VMEM((features, features), BF16),
            pltpu.VMEM((3, LANES, features), BF16),
            pltpu.VMEM((2, LANES, HEAD_DIM), F32),
            pltpu.VMEM((2 * planes, 8, 128), F32),
            pltpu.VMEM((planes, 2 * LANES, width), BF16),
            pltpu.VMEM((LANES, 512), F32),
            pltpu.VMEM((2, 2 * LANES, 512), F32),
            pltpu.VMEM((8, LANES, HEAD_DIM), BF16),
            pltpu.VMEM((2, 8, HEAD_DIM, LANES), BF16),
            pltpu.VMEM((2, 2, 2, keys, HEAD_DIM), BF16),
            pltpu.VMEM((2, 2, HEAD_DIM, keys), BF16),
            pltpu.VMEM((2, 2, keys, HEAD_DIM), F32),
            pltpu.VMEM((keys, LANES), F32),
            pltpu.VMEM((8, HEAD_DIM, LANES), BF16),
            pltpu.VMEM((keys, LANES), F32),
            pltpu.VMEM((keys, LANES), BF16),
            pltpu.VMEM((keys, LANES), BF16),
            pltpu.VMEM((2, 2, 2, far, 2 * rows, HEAD_DIM), BF16),
            pltpu.VMEM((2, 2, 2, far, 2 * rows, HEAD_DIM), BF16),
            pltpu.VMEM((8, LANES, HEAD_DIM), BF16),
            pltpu.VMEM((16, rows, HEAD_DIM), BF16),
            pltpu.VMEM((planes, rows, width), BF16),
            pltpu.VMEM((planes, rows, width), BF16),
            pltpu.VMEM((planes, LANES, width), F32),
            pltpu.VMEM((rows, features), BF16),
            pltpu.VMEM((rows, features), BF16),
            pltpu.VMEM((planes, width, 256), BF16),
            pltpu.VMEM((LANES, 256), BF16),
            pltpu.VMEM((rows, 256), BF16),
            pltpu.VMEM((planes, rows, width), BF16),
            dma((6,)),
            dma((14 + planes,)),
            dma((14 + planes,)),
            dma((5, 3, 2, far)),
            dma((5, 3, 2, far)),
            dma((2, 2, 2, far)),
            dma((2, 2, 2, far)),
            dma((8,)),
            dma((8,)),
            dma((2, planes)),
            dma((2, planes)),
            dma((planes,)),
            dma((planes,)),
        ],
        compiler_params=pltpu.CompilerParams(
            collective_id=0, has_side_effects=True, vmem_limit_bytes=67_043_328
        ),
        name="tick",
    )(xs[0], xf[0], dy[0], pos_tile, tables, gain, wq[0], wkv[0], wo[0])
    return produced[None], grads[None]


def solution(mesh):
    placed = (
        P("section", "ctx", None),
        P("section", "ctx", None),
        P("section", "ctx", None),
        P("ctx"),
        P("section", None),
        P("section", "ctx", None),
        P("section", "ctx", None),
        P("section", None, None),
    )
    return jax.shard_map(
        functools.partial(shards, mesh.shape["ctx"] // 2),
        mesh=mesh,
        in_specs=placed,
        out_specs=(P("section", "ctx", None), P("section", "ctx", None)),
        check_vma=False,
    )
```

```python
import functools

import jax
import jax.numpy as jnp
import numpy as np
from jax import lax
from jax.experimental import pallas as pl
from jax.experimental.pallas import tpu as pltpu
from jax.sharding import PartitionSpec as P

MESH = pl.DeviceIdType.MESH
F32 = jnp.float32
BF16 = jnp.bfloat16
HEAD_DIM = 128
LANES = 256
norm_eps = 1e-05
rope_base = 500000.0
LOG2E = 1.4426950408889634
HIDDEN = -1e30


def dot(a, b):
    return jnp.dot(a, b, preferred_element_type=F32)


def dot_nt(a, b):
    return lax.dot_general(a, b, (((1,), (1,)), ((), ())), preferred_element_type=F32)


def fold_rows(a, op):
    return op(a.reshape(a.shape[0] // 8, 8, a.shape[1]), axis=0)


def tick(
    planes,
    rows,
    xs_in,
    xf_in,
    dy_in,
    pos_in,
    freq_in,
    gain_in,
    wq_hbm,
    wkv_hbm,
    wo_hbm,
    next_out,
    grad_out,
    wkvb,
    wqb,
    wo,
    xbuf,
    tabs,
    posb,
    posown,
    normed,
    acc_kv,
    acc_q,
    qnat,
    qt,
    kv,
    kvt,
    dkv,
    bias,
    dmt,
    score,
    prob,
    dsc,
    stage,
    landed,
    mix,
    mixed,
    dnsend,
    dnrecv,
    dnown,
    fout,
    gout,
    wlent,
    last,
    lastrecv,
    loc_sem,
    x_send,
    x_recv,
    ring_send,
    ring_recv,
    rs_send,
    rs_recv,
    mix_send,
    mix_recv,
    out_send,
    out_recv,
):
    me = lax.axis_index("ctx")
    section = lax.axis_index("section")
    sections = lax.axis_size("section")
    z = me // 2
    h = me % 2
    partner = z * 2 + 1 - h
    to_z = (((z + 1) % planes) * 2 + h, ((z + planes - 1) % planes) * 2 + h)
    following = (section + 1) % sections
    preceding = (section + sections - 1) % sections
    width = wkvb.shape[1]
    half = width // 2
    pair = 2 * rows
    keys = planes * pair
    chunk = 256
    chunks = keys // chunk
    far = planes // 2
    mine = pl.ds(pl.multiple_of(h * rows, 16), rows)
    scale = HEAD_DIM ** (-0.5)
    scope = jax.named_scope

    barrier = pltpu.get_barrier_semaphore()
    for other in (partner, *to_z):
        pl.semaphore_signal(barrier, inc=1, device_id={"ctx": other}, device_id_type=MESH)
    core = section % 2
    f_side = core * (1 - h) + (1 - core) * h
    g_side = core * h + (1 - core) * (1 - h)
    f_rows, f_other = (pl.ds(pl.multiple_of(n * rows, 16), rows) for n in (f_side, 1 - f_side))
    g_rows, g_other = (pl.ds(pl.multiple_of(n * rows, 16), rows) for n in (g_side, 1 - g_side))
    f_to = {"section": following, "ctx": z * 2 + f_side}
    g_to = {"section": preceding, "ctx": z * 2 + g_side}
    for other in (f_to, g_to):
        pl.semaphore_signal(barrier, inc=1, device_id=other, device_id_type=MESH)

    def local(src, dst, n):
        return pltpu.make_async_copy(src, dst, loc_sem.at[n])

    def remote(src, dst, s, r, **to):
        return pltpu.make_async_remote_copy(
            src_ref=src, dst_ref=dst, send_sem=s, recv_sem=r, device_id=to, device_id_type=MESH
        )

    def to_partner(src, dst, n):
        return remote(src, dst, x_send.at[n], x_recv.at[n], ctx=partner)

    def plane(offset):
        return (z + 2 * planes + offset) % planes

    def pieces(side):
        pairs = []
        for n in range(2):
            at = pl.ds(pl.multiple_of(512 * n + side * 256, 256), 256)
            pairs.append((wkv_hbm.at[:, at], wkvb.at[z, my_rows, pl.ds(256 * n, 256)]))
        for j in range(2):
            at = pl.ds(pl.multiple_of(side * 1024 + j * 512, 512), 512)
            pairs.append((wq_hbm.at[:, at], wqb.at[j, z, my_rows, :]))
        return pairs

    my_rows = pl.ds(pl.multiple_of(h * half, 128), half)
    own = [local(src, dst, n) for n, (src, dst) in enumerate(pieces(h))]
    for c in own:
        c.start()
    load_wo = local(wo_hbm, wo, 4)
    load_wo.start()

    for n in range(3):
        xbuf[n, pl.ds(pair, LANES - pair), :] = jnp.zeros((LANES - pair, xbuf.shape[2]), BF16)
    tabs[:, pl.ds(pair, LANES - pair), :] = jnp.zeros((2, LANES - pair, HEAD_DIM), F32)
    where = jnp.concatenate([pos_in[...].astype(F32), jnp.zeros((1, 128 - rows), F32)], axis=1)
    posown[...] = jnp.broadcast_to(where, (8, 128))
    for n, src in enumerate((xs_in, xf_in, dy_in)):
        xbuf[n, mine, :] = src[...]
    for n in range(2):
        for k in range(2):
            dkv[n, k] = jnp.zeros((keys, HEAD_DIM), F32)

    posb[me] = posown[...]

    with scope("barrier"):
        pl.semaphore_wait(barrier, 5)

    given = pieces(1 - h)
    tokens = [(src, xbuf.at[n, mine, :]) for n, src in enumerate((xs_in, xf_in, dy_in))]
    swaps = [
        *given[:2],
        (posown, posb.at[me]),
        tokens[0],
        *given[2:],
        *tokens[1:],
    ]
    swap = [to_partner(src, dst, n) for n, (src, dst) in enumerate(swaps)]
    for c in swap:
        c.start()

    class Ring:
        def __init__(self, number, parts):
            self.number, self.parts = number, parts

        def copy(self, n, way, t):
            block = self.parts[n][0](plane(-t if way == 0 else t))
            sems = (self.number, n, way, t)
            return remote(block, block, ring_send.at[sems], ring_recv.at[sems], ctx=to_z[way])

        def step(self, t, ready=None, only=None):
            for n, (_, *hops) in enumerate(self.parts):
                if only is not None and n != only:
                    continue
                if t == 0 and ready is not None:
                    ready(n)
                for way in range(2):
                    if 0 < t <= hops[way]:
                        self.copy(n, way, t - 1).wait_recv()
                    if t < hops[way]:
                        self.copy(n, way, t).start()

        def sent(self):
            for n, (_, *hops) in enumerate(self.parts):
                for way in range(2):
                    for t in range(hops[way]):
                        self.copy(n, way, t).wait_send()

    def rows_of(ref, c):
        who = h if c == 0 else 1 - h
        at = pl.ds(pl.multiple_of(who * half, 128), half)
        return lambda p: ref.at[p, at, :]

    def w_parts(ref):
        return [(rows_of(ref, 0), far, far - 1), (rows_of(ref, 1), far - 1, far)]

    def kv_parts(m):
        def block(j):
            return lambda p: kv.at[m, j, :, pl.ds(pl.multiple_of(p * pair, 32), pair), :]

        return [(block(0), far, far - 1), (block(1), far - 1, far)]

    pos_part = (lambda p: posb.at[pl.ds(2 * p, 2)], far, far - 1)
    ring_wkv = Ring(0, [*w_parts(wkvb), pos_part])
    ring_q = [Ring(1 + j, w_parts(wqb.at[j])) for j in range(2)]
    ring_kv = [Ring(3 + m, kv_parts(m)) for m in range(2)]

    def ready_wkv(n):
        if n == 0:
            own[0].wait()
            own[1].wait()
        elif n == 1:
            swap[0].wait_recv()
            swap[1].wait_recv()
        else:
            swap[2].wait_recv()

    def ready_q(j):
        def ready(n):
            if n == 0:
                own[2 + j].wait()
            else:
                swap[4 + j].wait_recv()

        return ready

    def norms(n):
        def body(i, _):
            at = pl.ds(pl.multiple_of(i * 32, 32), 32)
            x = xbuf[n, at, :].astype(F32)
            inverse = lax.rsqrt(jnp.mean(x * x, axis=-1, keepdims=True) + norm_eps)
            y = (x * inverse * gain_in[...]).astype(BF16)
            for p in range(planes):
                normed[p, pl.ds(pl.multiple_of(n * LANES + i * 32, 32), 32), :] = y[:, p * width : (p + 1) * width]
            return 0

        lax.fori_loop(0, LANES // 32, body, 0)

    def project_kv(m):
        at = pl.ds(m * LANES, LANES)
        total = dot(normed[0, at, :], wkvb[0])
        for p in range(1, planes):
            total += dot(normed[p, at, :], wkvb[p])
        acc_kv[...] = total

    def project_q(j, offsets, first=False):
        ps = [plane(o) for o in offsets]
        total = dot(normed[ps[0]], wqb[j, ps[0]])
        for p in ps[1:]:
            total += dot(normed[p], wqb[j, p])
        if first:
            acc_q[j] = total
        else:
            acc_q[j] += total

    def grads_in():
        def body(n, _):
            at = pl.ds(pl.multiple_of(h * 1024 + n * 128, 128), 128)
            dmt[n] = dot_nt(wo[at, :], xbuf[2]).astype(BF16)
            return 0

        lax.fori_loop(0, 8, body, 0)

    def make_tables():
        lane = lax.broadcasted_iota(jnp.int32, (rows, HEAD_DIM), 1)
        for n in range(2):
            column = jnp.broadcast_to(posb[2 * z + n][0:1, :], (128, 128)).T[:rows]
            angles = column * freq_in[...]
            at = pl.ds(n * rows, rows)
            sine = jnp.sin(angles)
            tabs[0, at, :] = jnp.cos(angles)
            tabs[1, at, :] = jnp.where(lane < HEAD_DIM // 2, -sine, sine)

    def rotated(x, sign):
        return x * tabs[0] + sign * (pltpu.roll(x, HEAD_DIM // 2, 1) * tabs[1])

    at_z = pl.ds(pl.multiple_of(z * pair, 32), pair)

    def make_kv(m):
        for j in range(2):
            key = acc_kv[:, 128 * j : 128 * j + 128]
            kv[m, j, 0, at_z, :] = rotated(key, 1.0).astype(BF16)[:pair]
            kv[m, j, 1, at_z, :] = acc_kv[:, 256 + 128 * j : 384 + 128 * j].astype(BF16)[:pair]

    def make_q(j, m):
        for r in range(4):
            q = rotated(acc_q[j, m * LANES : (m + 1) * LANES, r * 128 : r * 128 + 128], 1.0)
            if m == 0:
                qnat[4 * j + r] = q.astype(BF16)
            qt[m, 4 * j + r] = q.T.astype(BF16)

    def make_bias():
        row0 = posb[2 * z][0:1, :]
        row1 = posb[2 * z + 1][0:1, :]
        zero = jnp.zeros_like(row0)
        wide0 = jnp.concatenate([row0, zero], axis=1)
        wide1 = pltpu.roll(jnp.concatenate([row1, zero], axis=1), rows, 1)
        lane = lax.broadcasted_iota(jnp.int32, (1, LANES), 1)
        query = jnp.where(lane < rows, wide0, jnp.where(lane < pair, wide1, 1e9))

        def body(i, _):
            column = jnp.broadcast_to(posb[i][0:1, :], (128, 128)).T
            column = jnp.concatenate([column, column], axis=1)[:rows]
            at = pl.ds(pl.multiple_of(i * rows, 16), rows)
            bias[at, :] = jnp.where(column <= query, 0.0, HIDDEN)
            return 0

        lax.fori_loop(0, 2 * planes, body, 0)

    def transposed(m, ks, js=(0, 1)):
        for j in js:
            for k in ks:
                for i in range(keys // 128):
                    at = pl.ds(i * 128, 128)
                    kvt[j, k, :, at] = kv[m, j, k, at, :].astype(F32).T.astype(BF16)

    def softmax(m, j, i):
        q = qt[m, i]
        top = jnp.full((8, LANES), HIDDEN, F32)
        for c in range(chunks):
            at = pl.ds(c * chunk, chunk)
            s = dot(kv[m, j, 0, at, :], q) + bias[at, :]
            score[at, :] = s
            top = jnp.maximum(top, fold_rows(s, jnp.max))
        top = jnp.max(top, axis=0, keepdims=True)
        total = jnp.zeros((8, LANES), F32)
        for c in range(chunks):
            at = pl.ds(c * chunk, chunk)
            e = jnp.exp2((score[at, :] - top) * (scale * LOG2E))
            total += fold_rows(e, jnp.sum)
            if m == 0:
                score[at, :] = e
            prob[at, :] = e.astype(BF16)
        return jnp.sum(total, axis=0, keepdims=True)

    def backward(j, i):
        inverse = 1.0 / softmax(0, j, i)
        summed = dot(kvt[j, 1], prob[...])
        dm = dmt[i].astype(F32)
        share = -jnp.sum(dm * summed, axis=0, keepdims=True) * (inverse * inverse)
        dsum = dm * inverse
        dsum_t = dsum.astype(BF16)
        dsum_n = dsum.T.astype(BF16)
        q = qnat[i]
        for c in range(chunks):
            at = pl.ds(c * chunk, chunk)
            dkv[j, 1, at, :] += dot(prob[at, :], dsum_n)
            ds = (score[at, :] * (dot(kv[0, j, 1, at, :], dsum_t) + share)).astype(BF16)
            dsc[at, :] = ds
            dkv[j, 0, at, :] += dot(ds, q) * scale
        dq = dot(kvt[j, 0], dsc[...]) * scale
        qnat[i] = dq.T.astype(BF16)

    def forward(j, i):
        inverse = 1.0 / softmax(1, j, i)
        mix[i] = (dot(kvt[j, 1], prob[...]) * inverse).T.astype(BF16)

    rs_hops = ((far - 1, far), (far, far - 1))

    def rs_copy(j, k, way, t):
        at = (j, k, way, t)
        return remote(stage.at[at], landed.at[at], rs_send.at[at], rs_recv.at[at], ctx=to_z[way])

    def rs_step(j, t):
        for k in range(2):
            for way in range(2):
                hops = rs_hops[k][way]
                if 0 < t <= hops:
                    rs_copy(j, k, way, t - 1).wait_recv()
                if t < hops:
                    p = plane(hops - t if way == 0 else t - hops)
                    part = dkv[j, k, pl.ds(pl.multiple_of(p * pair, 32), pair), :]
                    if t > 0:
                        part = part + landed[j, k, way, t - 1].astype(F32)
                    stage[j, k, way, t] = part.astype(BF16)
                    rs_copy(j, k, way, t).start()

    def in_order(i, **steps):
        for name, work in steps.items():
            pl.when(i == int(name[1:]))(work)

    def lend(k):
        at = pl.ds(k * (planes // 2), planes // 2)
        return to_partner(wkvb.at[at], wlent.at[at], 10 + k)

    with scope("a0"):
        ring_wkv.step(0, ready_wkv, 0)
        ring_q[0].step(0, ready_q(0), 0)
        ring_wkv.step(0, ready_wkv, 1)
        ring_wkv.step(0, ready_wkv, 2)
    with scope("a1"):
        ring_wkv.step(1)
    with scope("a2"):
        ring_wkv.step(2)
    with scope("a3"):
        ring_wkv.step(3)
    with scope("c0"):
        ring_q[0].step(1, None, 0)
        ring_q[0].step(0, ready_q(0), 1)
    with scope("norms0"):
        swap[3].wait_recv()
        norms(0)
        make_tables()
    with scope("a4"):
        ring_wkv.step(4)
    for k in range(2):
        lend(k).start()
    with scope("kv0"):
        project_kv(0)
        make_kv(0)
    ring_kv[0].step(0)
    with scope("c1"):
        ring_q[0].step(1, None, 1)
    with scope("b1"):
        ring_kv[0].step(1)
    with scope("bias"):
        make_bias()
    with scope("c2"):
        ring_q[0].step(2)
    with scope("b2"):
        ring_kv[0].step(2)
    with scope("norms1"):
        swap[6].wait_recv()
        norms(1)
    with scope("kv1"):
        project_kv(1)
        make_kv(1)
    with scope("c3"):
        ring_q[0].step(3)
    with scope("q0c"):
        project_q(0, (0, 1, -1, 2, -2, 3, -3), True)
    with scope("b3"):
        ring_kv[0].step(3)
    ring_q[1].step(0, ready_q(1))
    with scope("dm"):
        load_wo.wait()
        swap[7].wait_recv()
        grads_in()
    with scope("c4"):
        ring_q[0].step(4)
    with scope("q0d"):
        project_q(0, (4,))
        make_q(0, 0)
    with scope("b4"):
        ring_kv[0].step(4)
    with scope("t0"):
        transposed(0, (0, 1))

    def d_step(t, n):
        with scope(f"d{t}{n}"):
            ring_q[1].step(t, None, n)

    d_step(1, 0)

    def backward0(i, _):
        with scope("bwd"):
            backward(0, i)

        def third():
            d_step(2, 1)
            d_step(3, 0)

        in_order(i, i0=lambda: d_step(1, 1), i1=lambda: d_step(2, 0), i2=third, i3=lambda: d_step(3, 1))
        return 0

    lax.fori_loop(0, 4, backward0, 0)
    ring_kv[1].step(0)
    rs_step(0, 0)
    with scope("q1a"):
        project_q(1, (0, 1, -1, 2, -2, 3, -3), True)
        make_q(0, 1)
    with scope("d4"):
        ring_q[1].step(4)
    with scope("q1b"):
        project_q(1, (4,))
        make_q(1, 0)

    def f_step(t, j):
        with scope(f"f{t}{j}"):
            ring_kv[1].step(t, None, j)

    def g_step(j, t):
        with scope(f"g{j}{t}"):
            rs_step(j, t)

    def backward1(i, _):
        with scope("bwd"):
            backward(1, 4 + i)

        in_order(
            i,
            i0=lambda: f_step(1, 0),
            i1=lambda: f_step(1, 1),
            i2=lambda: g_step(0, 1),
            i3=lambda: f_step(2, 0),
        )
        return 0

    lax.fori_loop(0, 4, backward1, 0)
    rs_step(1, 0)

    def unrotated(x):
        return rotated(x, -1.0).astype(BF16)

    def owned(j):
        parts = []
        for k in range(2):
            part = dkv[j, k, at_z, :]
            for way in range(2):
                part = part + landed[j, k, way, rs_hops[k][way] - 1].astype(F32)
            part = part.astype(BF16).astype(F32)
            part = jnp.concatenate([part, jnp.zeros((LANES - pair, HEAD_DIM), F32)], axis=0)
            parts.append(unrotated(part) if k == 0 else part.astype(BF16))
        return jnp.concatenate(parts, axis=1)

    def dn_copy(p):
        return to_partner(dnsend.at[p], dnrecv.at[p], 14 + p)

    with scope("dq"):
        dq_all = [
            jnp.concatenate([unrotated(qnat[4 * j + r].astype(F32)) for r in range(4)], axis=1) for j in range(2)
        ]
    f_step(2, 1)

    def columns(ref, p, j):
        return jnp.concatenate(
            [ref[p, :, 128 * j : 128 * j + 128], ref[p, :, 256 + 128 * j : 384 + 128 * j]], axis=1
        )

    def dn_step(p, _):
        dnown[p] = dot_nt(dq_all[0], wqb[0, p]) + dot_nt(dq_all[1], wqb[1, p])
        dnsend[p] = dnown[p, g_other, :].astype(BF16)
        dn_copy(p).start()
        return 0

    def own_swap(j):
        return to_partner(last.at[j, g_other, :], lastrecv.at[j], 12 + j)

    def own_grads(j):
        with scope("dkv"):
            last[j] = owned(j)
        own_swap(j).start()

    def add_own(j):
        own_swap(j).wait_recv()
        own = last[j, g_rows, :]
        for p in range(planes):
            dnown[p, g_rows, :] += dot_nt(own, columns(wkvb, p, j)) + dot_nt(lastrecv[j], columns(wlent, p, j))

    with scope("dn"):
        lax.fori_loop(0, planes, dn_step, 0)
    g_step(0, 2)
    f_step(3, 0)
    g_step(1, 1)
    f_step(3, 1)
    f_step(4, 0)
    with scope("t1"):
        transposed(1, (1,), (0,))
        make_q(1, 1)

    def mix_copy(i):
        return remote(
            mix.at[i, f_other, :], mixed.at[8 * h + i], mix_send.at[i], mix_recv.at[i], ctx=partner
        )

    def forward_step(i, _):
        def group1():
            f_step(4, 1)
            with scope("t1"):
                transposed(1, (1,), (1,))

        in_order(i, i4=group1)
        with scope("fwd"):
            forward(i // 4, i)
        mix_copy(i).start()

        def fourth():
            g_step(0, 4)
            own_grads(0)

        def sixth():
            with scope("add0"):
                for k in range(2):
                    lend(k).wait_recv()
                add_own(0)

        in_order(
            i,
            i1=lambda: g_step(0, 3),
            i2=lambda: g_step(1, 2),
            i4=fourth,
            i5=lambda: g_step(1, 3),
            i6=sixth,
        )
        return 0

    lax.fori_loop(0, 8, forward_step, 0)

    with scope("g4"):
        rs_step(1, 4)
    own_grads(1)

    def out_copy(which, p):
        at = pl.ds(p * width, width)
        src, dst, to = ((fout, next_out, f_to), (gout, grad_out, g_to))[which]
        return remote(src.at[:, at], dst.at[:, at], out_send.at[which, p], out_recv.at[which, p], **to)

    with scope("out"):
        for n in range(8):
            mixed[8 * h + n] = mix[n, f_rows, :]
        for n in range(8):
            mix_copy(n).wait_recv()
        heads_all = jnp.concatenate([mixed[n] for n in range(16)], axis=1)
        for n in range(planes):
            at = pl.ds(n * width, width)
            fout[:, at] = (xbuf[1, f_rows, at].astype(F32) + dot(heads_all, wo[:, at])).astype(BF16)
            out_copy(0, n).start()

    x = xbuf[0, g_rows, :].astype(F32)
    inverse = lax.rsqrt(jnp.mean(x * x, axis=-1, keepdims=True) + norm_eps)
    along = jnp.zeros((rows, 1), F32)
    with scope("dnwait"):
        for p in range(planes):
            dn_copy(p).wait_recv()
        own_swap(1).wait_recv()
    with scope("last"):
        own_last = last[1, g_rows, :]
        for p in range(planes):
            at = slice(p * width, (p + 1) * width)
            total = dnown[p, g_rows, :] + dnrecv[p].astype(F32)
            total += dot_nt(own_last, columns(wkvb, p, 1)) + dot_nt(lastrecv[1], columns(wlent, p, 1))
            d = total.astype(BF16).astype(F32) * gain_in[:, at]
            dnown[p, g_rows, :] = d
            along += jnp.sum(d * x[:, at], axis=-1, keepdims=True)
    pull = along * (1.0 / x.shape[1]) * (inverse * inverse * inverse)
    with scope("grad"):
        for p in range(planes):
            at = slice(p * width, (p + 1) * width)
            grad = (dnown[p, g_rows, :] * inverse - x[:, at] * pull).astype(BF16)
            gout[:, at] = grad + xbuf[2, g_rows, at]
            out_copy(1, p).start()

    with scope("sent"):
        for c in (*swap, own_swap(0), own_swap(1), lend(0), lend(1), *(mix_copy(n) for n in range(8))):
            c.wait_send()
        for ring in (ring_wkv, *ring_q, *ring_kv):
            ring.sent()
        for j in range(2):
            for k in range(2):
                for way in range(2):
                    for t in range(rs_hops[k][way]):
                        rs_copy(j, k, way, t).wait_send()
        for p in range(planes):
            dn_copy(p).wait_send()
    with scope("outs"):
        for which in range(2):
            for p in range(planes):
                out_copy(which, p).wait()


def shards(planes, xf, xs, dy, positions, gain, wq, wkv, wo):
    rows, features = xf.shape[1:]
    keys = 2 * planes * rows
    width = features // planes
    frequency = rope_base ** (-2.0 * np.arange(HEAD_DIM // 2) / HEAD_DIM)
    frequency = jnp.asarray(np.tile(frequency, 2)[None, :], F32)
    vmem = pl.BlockSpec(memory_space=pltpu.VMEM)
    hbm = pl.BlockSpec(memory_space=pl.ANY)
    far = planes // 2
    dma = pltpu.SemaphoreType.DMA
    out = jax.ShapeDtypeStruct((rows, features), BF16)
    produced, grads = pl.pallas_call(
        functools.partial(tick, planes, rows),
        out_shape=(out, out),
        in_specs=[vmem] * 6 + [hbm] * 3,
        out_specs=(hbm, hbm),
        scratch_shapes=[
            pltpu.VMEM((planes, width, 512), BF16),
            pltpu.VMEM((2, planes, width, 512), BF16),
            pltpu.VMEM((features, features), BF16),
            pltpu.VMEM((3, LANES, features), BF16),
            pltpu.VMEM((2, LANES, HEAD_DIM), F32),
            pltpu.VMEM((2 * planes, 8, 128), F32),
            pltpu.VMEM((8, 128), F32),
            pltpu.VMEM((planes, 2 * LANES, width), BF16),
            pltpu.VMEM((LANES, 512), F32),
            pltpu.VMEM((2, 2 * LANES, 512), F32),
            pltpu.VMEM((8, LANES, HEAD_DIM), BF16),
            pltpu.VMEM((2, 8, HEAD_DIM, LANES), BF16),
            pltpu.VMEM((2, 2, 2, keys, HEAD_DIM), BF16),
            pltpu.VMEM((2, 2, HEAD_DIM, keys), BF16),
            pltpu.VMEM((2, 2, keys, HEAD_DIM), F32),
            pltpu.VMEM((keys, LANES), F32),
            pltpu.VMEM((8, HEAD_DIM, LANES), BF16),
            pltpu.VMEM((keys, LANES), F32),
            pltpu.VMEM((keys, LANES), BF16),
            pltpu.VMEM((keys, LANES), BF16),
            pltpu.VMEM((2, 2, 2, far, 2 * rows, HEAD_DIM), BF16),
            pltpu.VMEM((2, 2, 2, far, 2 * rows, HEAD_DIM), BF16),
            pltpu.VMEM((8, LANES, HEAD_DIM), BF16),
            pltpu.VMEM((16, rows, HEAD_DIM), BF16),
            pltpu.VMEM((planes, rows, width), BF16),
            pltpu.VMEM((planes, rows, width), BF16),
            pltpu.VMEM((planes, LANES, width), F32),
            pltpu.VMEM((rows, features), BF16),
            pltpu.VMEM((rows, features), BF16),
            pltpu.VMEM((planes, width, 512), BF16),
            pltpu.VMEM((2, LANES, 256), BF16),
            pltpu.VMEM((2, rows, 256), BF16),
            dma((6,)),
            dma((14 + planes,)),
            dma((14 + planes,)),
            dma((5, 3, 2, far)),
            dma((5, 3, 2, far)),
            dma((2, 2, 2, far)),
            dma((2, 2, 2, far)),
            dma((8,)),
            dma((8,)),
            dma((2, planes)),
            dma((2, planes)),
        ],
        compiler_params=pltpu.CompilerParams(
            collective_id=0, has_side_effects=True, vmem_limit_bytes=52 * 2**20
        ),
        name="tick",
    )(xs[0], xf[0], dy[0], positions[None, :], frequency, gain, wq[0], wkv[0], wo[0])
    return produced[None], grads[None]


def solution(mesh):
    placed = (
        P("section", "ctx", None),
        P("section", "ctx", None),
        P("section", "ctx", None),
        P("ctx"),
        P("section", None),
        P("section", "ctx", None),
        P("section", "ctx", None),
        P("section", None, None),
    )
    return jax.shard_map(
        functools.partial(shards, mesh.shape["ctx"] // 2),
        mesh=mesh,
        in_specs=placed,
        out_specs=(P("section", "ctx", None), P("section", "ctx", None)),
        check_vma=False,
    )
```

```python
import functools

import jax
import jax.numpy as jnp
import numpy as np
from jax import lax
from jax.experimental import pallas as pl
from jax.experimental.pallas import tpu as pltpu
from jax.sharding import PartitionSpec as P

MESH = pl.DeviceIdType.MESH
F32 = jnp.float32
BF16 = jnp.bfloat16
HEAD_DIM = 128
LANES = 256
norm_eps = 1e-05
rope_base = 500000.0
LOG2E = 1.4426950408889634
HIDDEN = -1e30


def dot(a, b):
    return jnp.dot(a, b, preferred_element_type=F32)


def dot_nt(a, b):
    return lax.dot_general(a, b, (((1,), (1,)), ((), ())), preferred_element_type=F32)


def fold_rows(a, op):
    return op(a.reshape(a.shape[0] // 8, 8, a.shape[1]), axis=0)


def tick(
    planes,
    rows,
    xs_in,
    xf_in,
    dy_in,
    pos_in,
    freq_in,
    gain_in,
    wq_hbm,
    wkv_hbm,
    wo_hbm,
    next_out,
    grad_out,
    wkvb,
    wqb,
    wo,
    xbuf,
    tabs,
    posb,
    posown,
    normed,
    acc_kv,
    acc_q,
    qnat,
    qt,
    kv,
    kvt,
    dkv,
    bias,
    dmt,
    score,
    prob,
    dsc,
    stage,
    landed,
    mix,
    mixed,
    dnsend,
    dnrecv,
    dnown,
    fout,
    gout,
    wlent,
    last,
    lastrecv,
    loc_sem,
    x_send,
    x_recv,
    ring_send,
    ring_recv,
    rs_send,
    rs_recv,
    mix_send,
    mix_recv,
    out_send,
    out_recv,
):
    me = lax.axis_index("ctx")
    section = lax.axis_index("section")
    sections = lax.axis_size("section")
    z = me // 2
    h = me % 2
    partner = z * 2 + 1 - h
    to_z = (((z + 1) % planes) * 2 + h, ((z + planes - 1) % planes) * 2 + h)
    following = (section + 1) % sections
    preceding = (section + sections - 1) % sections
    width = wkvb.shape[1]
    half = width // 2
    pair = 2 * rows
    keys = planes * pair
    chunk = 256
    chunks = keys // chunk
    far = planes // 2
    mine = pl.ds(pl.multiple_of(h * rows, 16), rows)
    scale = HEAD_DIM ** (-0.5)
    scope = jax.named_scope

    barrier = pltpu.get_barrier_semaphore()
    for other in (partner, *to_z):
        pl.semaphore_signal(barrier, inc=1, device_id={"ctx": other}, device_id_type=MESH)
    core = section % 2
    f_side = core * (1 - h) + (1 - core) * h
    g_side = core * h + (1 - core) * (1 - h)
    f_rows, f_other = (pl.ds(pl.multiple_of(n * rows, 16), rows) for n in (f_side, 1 - f_side))
    g_rows, g_other = (pl.ds(pl.multiple_of(n * rows, 16), rows) for n in (g_side, 1 - g_side))
    f_to = {"section": following, "ctx": z * 2 + f_side}
    g_to = {"section": preceding, "ctx": z * 2 + g_side}
    for other in (f_to, g_to):
        pl.semaphore_signal(barrier, inc=1, device_id=other, device_id_type=MESH)

    def local(src, dst, n):
        return pltpu.make_async_copy(src, dst, loc_sem.at[n])

    def remote(src, dst, s, r, **to):
        return pltpu.make_async_remote_copy(
            src_ref=src, dst_ref=dst, send_sem=s, recv_sem=r, device_id=to, device_id_type=MESH
        )

    def to_partner(src, dst, n):
        return remote(src, dst, x_send.at[n], x_recv.at[n], ctx=partner)

    def plane(offset):
        return (z + 2 * planes + offset) % planes

    def pieces(side):
        pairs = []
        for n in range(2):
            at = pl.ds(pl.multiple_of(512 * n + side * 256, 256), 256)
            pairs.append((wkv_hbm.at[:, at], wkvb.at[z, my_rows, pl.ds(256 * n, 256)]))
        for j in range(2):
            at = pl.ds(pl.multiple_of(side * 1024 + j * 512, 512), 512)
            pairs.append((wq_hbm.at[:, at], wqb.at[j, z, my_rows, :]))
        return pairs

    my_rows = pl.ds(pl.multiple_of(h * half, 128), half)
    own = [local(src, dst, n) for n, (src, dst) in enumerate(pieces(h))]
    for c in own:
        c.start()
    load_wo = local(wo_hbm, wo, 4)
    load_wo.start()

    for n in range(3):
        xbuf[n, pl.ds(pair, LANES - pair), :] = jnp.zeros((LANES - pair, xbuf.shape[2]), BF16)
    tabs[:, pl.ds(pair, LANES - pair), :] = jnp.zeros((2, LANES - pair, HEAD_DIM), F32)
    where = jnp.concatenate([pos_in[...].astype(F32), jnp.zeros((1, 128 - rows), F32)], axis=1)
    posown[...] = jnp.broadcast_to(where, (8, 128))
    for n, src in enumerate((xs_in, xf_in, dy_in)):
        xbuf[n, mine, :] = src[...]
    for n in range(2):
        for k in range(2):
            dkv[n, k] = jnp.zeros((keys, HEAD_DIM), F32)

    posb[me] = posown[...]

    with scope("barrier"):
        pl.semaphore_wait(barrier, 5)

    given = pieces(1 - h)
    tokens = [(src, xbuf.at[n, mine, :]) for n, src in enumerate((xs_in, xf_in, dy_in))]
    swaps = [
        *given[:2],
        (posown, posb.at[me]),
        tokens[0],
        *given[2:],
        *tokens[1:],
    ]
    swap = [to_partner(src, dst, n) for n, (src, dst) in enumerate(swaps)]
    for c in swap:
        c.start()

    class Ring:
        def __init__(self, number, parts):
            self.number, self.parts = number, parts

        def copy(self, n, way, t):
            block = self.parts[n][0](plane(-t if way == 0 else t))
            sems = (self.number, n, way, t)
            return remote(block, block, ring_send.at[self.number], ring_recv.at[sems], ctx=to_z[way])

        def step(self, t, ready=None, only=None):
            for n, (_, *hops) in enumerate(self.parts):
                if only is not None and n != only:
                    continue
                if t == 0 and ready is not None:
                    ready(n)
                for way in range(2):
                    if 0 < t <= hops[way]:
                        self.copy(n, way, t - 1).wait_recv()
                    if t < hops[way]:
                        self.copy(n, way, t).start()

    def rows_of(ref, c):
        who = h if c == 0 else 1 - h
        at = pl.ds(pl.multiple_of(who * half, 128), half)
        return lambda p: ref.at[p, at, :]

    def w_parts(ref):
        return [(rows_of(ref, 0), far, far - 1), (rows_of(ref, 1), far - 1, far)]

    def kv_parts(m):
        def block(j):
            return lambda p: kv.at[m, j, :, pl.ds(pl.multiple_of(p * pair, 32), pair), :]

        return [(block(0), far, far - 1), (block(1), far - 1, far)]

    pos_part = (lambda p: posb.at[pl.ds(2 * p, 2)], far, far - 1)
    ring_wkv = Ring(0, w_parts(wkvb))
    ring_pos = Ring(5, [pos_part])
    ring_q = [Ring(1 + j, w_parts(wqb.at[j])) for j in range(2)]
    ring_kv = [Ring(3 + m, kv_parts(m)) for m in range(2)]

    def ready_wkv(n):
        if n == 0:
            own[0].wait()
            own[1].wait()
        elif n == 1:
            swap[0].wait_recv()
            swap[1].wait_recv()

    def ready_pos(n):
        swap[2].wait_recv()

    def ready_q(j):
        def ready(n):
            if n == 0:
                own[2 + j].wait()
            else:
                swap[4 + j].wait_recv()

        return ready

    def norms(n):
        def body(i, _):
            at = pl.ds(pl.multiple_of(i * 32, 32), 32)
            x = xbuf[n, at, :].astype(F32)
            inverse = lax.rsqrt(jnp.mean(x * x, axis=-1, keepdims=True) + norm_eps)
            y = (x * inverse * gain_in[...]).astype(BF16)
            for p in range(planes):
                normed[p, pl.ds(pl.multiple_of(n * LANES + i * 32, 32), 32), :] = y[:, p * width : (p + 1) * width]
            return 0

        lax.fori_loop(0, LANES // 32, body, 0)

    def project_kv(m):
        at = pl.ds(m * LANES, LANES)
        total = dot(normed[0, at, :], wkvb[0])
        for p in range(1, planes):
            total += dot(normed[p, at, :], wkvb[p])
        acc_kv[...] = total

    def project_q(j, offsets, first=False):
        ps = [plane(o) for o in offsets]
        total = dot(normed[ps[0]], wqb[j, ps[0]])
        for p in ps[1:]:
            total += dot(normed[p], wqb[j, p])
        if first:
            acc_q[j] = total
        else:
            acc_q[j] += total

    def grads_in():
        def body(n, _):
            at = pl.ds(pl.multiple_of(h * 1024 + n * 128, 128), 128)
            dmt[n] = dot_nt(wo[at, :], xbuf[2]).astype(BF16)
            return 0

        lax.fori_loop(0, 8, body, 0)

    def make_tables():
        lane = lax.broadcasted_iota(jnp.int32, (rows, HEAD_DIM), 1)
        for n in range(2):
            column = jnp.broadcast_to(posb[2 * z + n][0:1, :], (128, 128)).T[:rows]
            angles = column * freq_in[...]
            at = pl.ds(n * rows, rows)
            sine = jnp.sin(angles)
            tabs[0, at, :] = jnp.cos(angles)
            tabs[1, at, :] = jnp.where(lane < HEAD_DIM // 2, -sine, sine)

    def rotated(x, sign):
        return x * tabs[0] + sign * (pltpu.roll(x, HEAD_DIM // 2, 1) * tabs[1])

    at_z = pl.ds(pl.multiple_of(z * pair, 32), pair)

    def make_kv(m):
        for j in range(2):
            key = acc_kv[:, 128 * j : 128 * j + 128]
            kv[m, j, 0, at_z, :] = rotated(key, 1.0).astype(BF16)[:pair]
            kv[m, j, 1, at_z, :] = acc_kv[:, 256 + 128 * j : 384 + 128 * j].astype(BF16)[:pair]

    def make_q(j, m):
        for r in range(4):
            q = rotated(acc_q[j, m * LANES : (m + 1) * LANES, r * 128 : r * 128 + 128], 1.0)
            if m == 0:
                qnat[4 * j + r] = q.astype(BF16)
            qt[m, 4 * j + r] = q.T.astype(BF16)

    def make_bias():
        row0 = posb[2 * z][0:1, :]
        row1 = posb[2 * z + 1][0:1, :]
        zero = jnp.zeros_like(row0)
        wide0 = jnp.concatenate([row0, zero], axis=1)
        wide1 = pltpu.roll(jnp.concatenate([row1, zero], axis=1), rows, 1)
        lane = lax.broadcasted_iota(jnp.int32, (1, LANES), 1)
        query = jnp.where(lane < rows, wide0, jnp.where(lane < pair, wide1, 1e9))

        def body(i, _):
            column = jnp.broadcast_to(posb[i][0:1, :], (128, 128)).T
            column = jnp.concatenate([column, column], axis=1)[:rows]
            at = pl.ds(pl.multiple_of(i * rows, 16), rows)
            bias[at, :] = jnp.where(column <= query, 0.0, HIDDEN)
            return 0

        lax.fori_loop(0, 2 * planes, body, 0)

    def transposed(m, ks, js=(0, 1)):
        for j in js:
            for k in ks:
                for i in range(keys // 128):
                    at = pl.ds(i * 128, 128)
                    kvt[j, k, :, at] = kv[m, j, k, at, :].astype(F32).T.astype(BF16)

    def softmax(m, j, i):
        q = qt[m, i]
        top = jnp.full((8, LANES), HIDDEN, F32)
        for c in range(chunks):
            at = pl.ds(c * chunk, chunk)
            s = dot(kv[m, j, 0, at, :], q) + bias[at, :]
            score[at, :] = s
            top = jnp.maximum(top, fold_rows(s, jnp.max))
        top = jnp.max(top, axis=0, keepdims=True)
        total = jnp.zeros((8, LANES), F32)
        for c in range(chunks):
            at = pl.ds(c * chunk, chunk)
            e = jnp.exp2((score[at, :] - top) * (scale * LOG2E))
            total += fold_rows(e, jnp.sum)
            if m == 0:
                score[at, :] = e
            prob[at, :] = e.astype(BF16)
        return jnp.sum(total, axis=0, keepdims=True)

    def backward(j, i):
        inverse = 1.0 / softmax(0, j, i)
        summed = dot(kvt[j, 1], prob[...])
        dm = dmt[i].astype(F32)
        share = -jnp.sum(dm * summed, axis=0, keepdims=True) * (inverse * inverse)
        dsum = dm * inverse
        dsum_t = dsum.astype(BF16)
        dsum_n = dsum.T.astype(BF16)
        q = qnat[i]
        for c in range(chunks):
            at = pl.ds(c * chunk, chunk)
            dkv[j, 1, at, :] += dot(prob[at, :], dsum_n)
            ds = (score[at, :] * (dot(kv[0, j, 1, at, :], dsum_t) + share)).astype(BF16)
            dsc[at, :] = ds
            dkv[j, 0, at, :] += dot(ds, q) * scale
        dq = dot(kvt[j, 0], dsc[...]) * scale
        qnat[i] = dq.T.astype(BF16)

    def forward(j, i):
        inverse = 1.0 / softmax(1, j, i)
        mix[i] = (dot(kvt[j, 1], prob[...]) * inverse).T.astype(BF16)

    rs_hops = ((far - 1, far), (far, far - 1))

    def rs_copy(j, k, way, t):
        at = (j, k, way, t)
        return remote(stage.at[at], landed.at[at], rs_send.at[j], rs_recv.at[at], ctx=to_z[way])

    def rs_step(j, t):
        for k in range(2):
            for way in range(2):
                hops = rs_hops[k][way]
                if 0 < t <= hops:
                    rs_copy(j, k, way, t - 1).wait_recv()
                if t < hops:
                    p = plane(hops - t if way == 0 else t - hops)
                    part = dkv[j, k, pl.ds(pl.multiple_of(p * pair, 32), pair), :]
                    if t > 0:
                        part = part + landed[j, k, way, t - 1].astype(F32)
                    stage[j, k, way, t] = part.astype(BF16)
                    rs_copy(j, k, way, t).start()

    def in_order(i, **steps):
        for name, work in steps.items():
            pl.when(i == int(name[1:]))(work)

    def lend(k):
        at = pl.ds(k * (planes // 2), planes // 2)
        return to_partner(wkvb.at[at], wlent.at[at], 10 + k)

    with scope("a0"):
        ring_wkv.step(0, ready_wkv, 0)
        ring_q[0].step(0, ready_q(0), 0)
        ring_wkv.step(0, ready_wkv, 1)
        ring_pos.step(0, ready_pos)
    with scope("a1"):
        ring_wkv.step(1)
        ring_pos.step(1)
    with scope("a2"):
        ring_wkv.step(2)
        ring_pos.step(2)
    with scope("a3"):
        ring_wkv.step(3)
        ring_pos.step(3)
    with scope("c0"):
        ring_q[0].step(1, None, 0)
        ring_q[0].step(0, ready_q(0), 1)
    with scope("norms0"):
        swap[3].wait_recv()
        norms(0)
        make_tables()
    with scope("a4"):
        ring_wkv.step(4)
        ring_pos.step(4)
    for k in range(2):
        lend(k).start()
    with scope("kv0"):
        project_kv(0)
        make_kv(0)
    ring_kv[0].step(0)
    with scope("c1"):
        ring_q[0].step(1, None, 1)
    with scope("b1"):
        ring_kv[0].step(1)
    with scope("bias"):
        make_bias()
    with scope("c2"):
        ring_q[0].step(2)
    with scope("b2"):
        ring_kv[0].step(2)
    with scope("norms1"):
        swap[6].wait_recv()
        norms(1)
    with scope("kv1"):
        project_kv(1)
        make_kv(1)
    with scope("c3"):
        ring_q[0].step(3)
    with scope("q0c"):
        project_q(0, (0, 1, -1, 2, -2, 3, -3), True)
    with scope("b3"):
        ring_kv[0].step(3)
    ring_q[1].step(0, ready_q(1))
    with scope("dm"):
        load_wo.wait()
        swap[7].wait_recv()
        grads_in()
    with scope("c4"):
        ring_q[0].step(4)
    with scope("q0d"):
        project_q(0, (4,))
        make_q(0, 0)
    with scope("b4"):
        ring_kv[0].step(4)
    with scope("t0"):
        transposed(0, (0, 1))

    def d_step(t, n):
        with scope(f"d{t}{n}"):
            ring_q[1].step(t, None, n)

    d_step(1, 0)

    def backward0(i, _):
        with scope("bwd"):
            backward(0, i)

        def third():
            d_step(2, 1)
            d_step(3, 0)

        in_order(i, i0=lambda: d_step(1, 1), i1=lambda: d_step(2, 0), i2=third, i3=lambda: d_step(3, 1))
        return 0

    lax.fori_loop(0, 4, backward0, 0)
    ring_kv[1].step(0)
    rs_step(0, 0)
    with scope("q1a"):
        project_q(1, (0, 1, -1, 2, -2, 3, -3), True)
        make_q(0, 1)
    with scope("d4"):
        ring_q[1].step(4)
    with scope("q1b"):
        project_q(1, (4,))
        make_q(1, 0)

    def f_step(t, j):
        with scope(f"f{t}{j}"):
            ring_kv[1].step(t, None, j)

    def g_step(j, t):
        with scope(f"g{j}{t}"):
            rs_step(j, t)

    def backward1(i, _):
        with scope("bwd"):
            backward(1, 4 + i)

        in_order(
            i,
            i0=lambda: f_step(1, 0),
            i1=lambda: f_step(1, 1),
            i2=lambda: g_step(0, 1),
            i3=lambda: f_step(2, 0),
        )
        return 0

    lax.fori_loop(0, 4, backward1, 0)
    rs_step(1, 0)

    def unrotated(x):
        return rotated(x, -1.0).astype(BF16)

    def owned(j):
        parts = []
        for k in range(2):
            part = dkv[j, k, at_z, :]
            for way in range(2):
                part = part + landed[j, k, way, rs_hops[k][way] - 1].astype(F32)
            part = part.astype(BF16).astype(F32)
            part = jnp.concatenate([part, jnp.zeros((LANES - pair, HEAD_DIM), F32)], axis=0)
            parts.append(unrotated(part) if k == 0 else part.astype(BF16))
        return jnp.concatenate(parts, axis=1)

    def dn_copy(p):
        return to_partner(dnsend.at[p], dnrecv.at[p], 14 + p)

    with scope("dq"):
        dq_all = [
            jnp.concatenate([unrotated(qnat[4 * j + r].astype(F32)) for r in range(4)], axis=1) for j in range(2)
        ]
    f_step(2, 1)

    def columns(ref, p, j):
        return jnp.concatenate(
            [ref[p, :, 128 * j : 128 * j + 128], ref[p, :, 256 + 128 * j : 384 + 128 * j]], axis=1
        )

    def dn_step(p, _):
        dnown[p] = dot_nt(dq_all[0], wqb[0, p]) + dot_nt(dq_all[1], wqb[1, p])
        dnsend[p] = dnown[p, g_other, :].astype(BF16)
        dn_copy(p).start()
        return 0

    def own_swap(j):
        return to_partner(last.at[j, g_other, :], lastrecv.at[j], 12 + j)

    def own_grads(j):
        with scope("dkv"):
            last[j] = owned(j)
        own_swap(j).start()

    def add_own(j):
        own_swap(j).wait_recv()
        own = last[j, g_rows, :]
        for p in range(planes):
            dnown[p, g_rows, :] += dot_nt(own, columns(wkvb, p, j)) + dot_nt(lastrecv[j], columns(wlent, p, j))

    with scope("dn"):
        lax.fori_loop(0, planes, dn_step, 0)
    g_step(0, 2)
    f_step(3, 0)
    g_step(1, 1)
    f_step(3, 1)
    f_step(4, 0)
    with scope("t1"):
        transposed(1, (1,), (0,))
        make_q(1, 1)

    def mix_copy(i):
        return remote(
            mix.at[i, f_other, :], mixed.at[8 * h + i], mix_send.at[i], mix_recv.at[i], ctx=partner
        )

    def forward_step(i, _):
        def group1():
            f_step(4, 1)
            with scope("t1"):
                transposed(1, (1,), (1,))

        in_order(i, i4=group1)
        with scope("fwd"):
            forward(i // 4, i)
        mix_copy(i).start()

        def fourth():
            g_step(0, 4)
            own_grads(0)

        def sixth():
            with scope("add0"):
                for k in range(2):
                    lend(k).wait_recv()
                add_own(0)

        in_order(
            i,
            i1=lambda: g_step(0, 3),
            i2=lambda: g_step(1, 2),
            i4=fourth,
            i5=lambda: g_step(1, 3),
            i6=sixth,
        )
        return 0

    lax.fori_loop(0, 8, forward_step, 0)

    with scope("g4"):
        rs_step(1, 4)
    own_grads(1)

    def out_copy(which, p):
        at = pl.ds(p * width, width)
        src, dst, to = ((fout, next_out, f_to), (gout, grad_out, g_to))[which]
        return remote(src.at[:, at], dst.at[:, at], out_send.at[which], out_recv.at[which], **to)

    with scope("out"):
        for n in range(8):
            mixed[8 * h + n] = mix[n, f_rows, :]
        for n in range(8):
            mix_copy(n).wait_recv()
        heads_all = jnp.concatenate([mixed[n] for n in range(16)], axis=1)
        for n in range(planes):
            at = pl.ds(n * width, width)
            fout[:, at] = (xbuf[1, f_rows, at].astype(F32) + dot(heads_all, wo[:, at])).astype(BF16)
            out_copy(0, n).start()

    x = xbuf[0, g_rows, :].astype(F32)
    inverse = lax.rsqrt(jnp.mean(x * x, axis=-1, keepdims=True) + norm_eps)
    along = jnp.zeros((rows, 1), F32)
    with scope("dnwait"):
        for p in range(planes):
            dn_copy(p).wait_recv()
        own_swap(1).wait_recv()
    with scope("last"):
        own_last = last[1, g_rows, :]
        for p in range(planes):
            at = slice(p * width, (p + 1) * width)
            total = dnown[p, g_rows, :] + dnrecv[p].astype(F32)
            total += dot_nt(own_last, columns(wkvb, p, 1)) + dot_nt(lastrecv[1], columns(wlent, p, 1))
            d = total.astype(BF16).astype(F32) * gain_in[:, at]
            dnown[p, g_rows, :] = d
            along += jnp.sum(d * x[:, at], axis=-1, keepdims=True)
    pull = along * (1.0 / x.shape[1]) * (inverse * inverse * inverse)
    with scope("grad"):
        for p in range(planes):
            at = slice(p * width, (p + 1) * width)
            grad = (dnown[p, g_rows, :] * inverse - x[:, at] * pull).astype(BF16)
            gout[:, at] = grad + xbuf[2, g_rows, at]
            out_copy(1, p).start()

    with scope("sent"):
        for c in (*swap, own_swap(0), own_swap(1), lend(0), lend(1), *(mix_copy(n) for n in range(8))):
            c.wait_send()
        most = pl.ds(0, planes - 1)
        many = pl.ds(0, (planes - 1) * pair)
        whole = [
            (wkvb.at[most], ring_send.at[0]),
            (posb.at[pl.ds(0, 2 * planes - 2)], ring_send.at[5]),
            (wqb.at[0, most], ring_send.at[1]),
            (wqb.at[1, most], ring_send.at[2]),
            (kv.at[0, :, :, many, :], ring_send.at[3]),
            (kv.at[1, :, :, many, :], ring_send.at[4]),
            (kv.at[0, 0, :, many, :], rs_send.at[0]),
            (kv.at[0, 0, :, many, :], rs_send.at[1]),
            (fout, out_send.at[0]),
            (gout, out_send.at[1]),
        ]
        for ref, sem in whole:
            remote(ref, ref, sem, sem, ctx=partner).wait_send()
        for p in range(planes):
            dn_copy(p).wait_send()
    with scope("outs"):
        for which, (ref, out, to) in enumerate(((fout, next_out, f_to), (gout, grad_out, g_to))):
            remote(ref, out, out_send.at[which], out_recv.at[which], **to).wait_recv()


def shards(planes, xf, xs, dy, positions, gain, wq, wkv, wo):
    rows, features = xf.shape[1:]
    keys = 2 * planes * rows
    width = features // planes
    frequency = rope_base ** (-2.0 * np.arange(HEAD_DIM // 2) / HEAD_DIM)
    frequency = jnp.asarray(np.tile(frequency, 2)[None, :], F32)
    vmem = pl.BlockSpec(memory_space=pltpu.VMEM)
    hbm = pl.BlockSpec(memory_space=pl.ANY)
    far = planes // 2
    dma = pltpu.SemaphoreType.DMA
    out = jax.ShapeDtypeStruct((rows, features), BF16)
    produced, grads = pl.pallas_call(
        functools.partial(tick, planes, rows),
        out_shape=(out, out),
        in_specs=[vmem] * 6 + [hbm] * 3,
        out_specs=(hbm, hbm),
        scratch_shapes=[
            pltpu.VMEM((planes, width, 512), BF16),
            pltpu.VMEM((2, planes, width, 512), BF16),
            pltpu.VMEM((features, features), BF16),
            pltpu.VMEM((3, LANES, features), BF16),
            pltpu.VMEM((2, LANES, HEAD_DIM), F32),
            pltpu.VMEM((2 * planes, 8, 128), F32),
            pltpu.VMEM((8, 128), F32),
            pltpu.VMEM((planes, 2 * LANES, width), BF16),
            pltpu.VMEM((LANES, 512), F32),
            pltpu.VMEM((2, 2 * LANES, 512), F32),
            pltpu.VMEM((8, LANES, HEAD_DIM), BF16),
            pltpu.VMEM((2, 8, HEAD_DIM, LANES), BF16),
            pltpu.VMEM((2, 2, 2, keys, HEAD_DIM), BF16),
            pltpu.VMEM((2, 2, HEAD_DIM, keys), BF16),
            pltpu.VMEM((2, 2, keys, HEAD_DIM), F32),
            pltpu.VMEM((keys, LANES), F32),
            pltpu.VMEM((8, HEAD_DIM, LANES), BF16),
            pltpu.VMEM((keys, LANES), F32),
            pltpu.VMEM((keys, LANES), BF16),
            pltpu.VMEM((keys, LANES), BF16),
            pltpu.VMEM((2, 2, 2, far, 2 * rows, HEAD_DIM), BF16),
            pltpu.VMEM((2, 2, 2, far, 2 * rows, HEAD_DIM), BF16),
            pltpu.VMEM((8, LANES, HEAD_DIM), BF16),
            pltpu.VMEM((16, rows, HEAD_DIM), BF16),
            pltpu.VMEM((planes, rows, width), BF16),
            pltpu.VMEM((planes, rows, width), BF16),
            pltpu.VMEM((planes, LANES, width), F32),
            pltpu.VMEM((rows, features), BF16),
            pltpu.VMEM((rows, features), BF16),
            pltpu.VMEM((planes, width, 512), BF16),
            pltpu.VMEM((2, LANES, 256), BF16),
            pltpu.VMEM((2, rows, 256), BF16),
            dma((6,)),
            dma((14 + planes,)),
            dma((14 + planes,)),
            dma((6,)),
            dma((6, 2, 2, far)),
            dma((2,)),
            dma((2, 2, 2, far)),
            dma((8,)),
            dma((8,)),
            dma((2,)),
            dma((2,)),
        ],
        compiler_params=pltpu.CompilerParams(
            collective_id=0, has_side_effects=True, vmem_limit_bytes=52 * 2**20
        ),
        name="tick",
    )(xs[0], xf[0], dy[0], positions[None, :], frequency, gain, wq[0], wkv[0], wo[0])
    return produced[None], grads[None]


def solution(mesh):
    placed = (
        P("section", "ctx", None),
        P("section", "ctx", None),
        P("section", "ctx", None),
        P("ctx"),
        P("section", None),
        P("section", "ctx", None),
        P("section", "ctx", None),
        P("section", None, None),
    )
    return jax.shard_map(
        functools.partial(shards, mesh.shape["ctx"] // 2),
        mesh=mesh,
        in_specs=placed,
        out_specs=(P("section", "ctx", None), P("section", "ctx", None)),
        check_vma=False,
    )
```
